32 devices in a mesh: grp: 2 (over y), tm: 16 (over z, x, core).
Axes of the slice: x: 2, y: 2, z: 4, core: 2. Of those that a mesh axis runs over, the one named last changes fastest.
Arguments:
- traces: float32 [2048, 16384], P('grp', 'tm'), parts along dimension 0, may hold values from -6 to 6
- templates: float32 [64, 8192], P('tm'), may hold values from -6 to 6
- moveouts: int32 [2048], P('grp'), parts along dimension 0, may hold values from 0 to 2047
- masks: int32 [64, 2048], P(None, 'grp'), parts along dimension 1, may hold values 0 or 1
Outputs:
- detection: float32 [64, 16384], P('tm', 'grp'), parts along dimension 1
The draws below stay inside these ranges and needn't reach their ends.
There are 2 independent parts, one for each index of `grp`. The reference program is written for one: setup_inputs(seed, part) draws one part's arguments, and reference() takes and returns one part's arrays. A program takes and returns all parts, laid end to end along the dimension named above; an argument that names none is the same for every part. Nothing has to cross between parts.
All inputs are finite; a program needn't handle non-finite values.
Results may differ from the reference program's by a relative error of at most 0.000073.
Values sent between devices are 32-bit elements; how exact they have to be, the bound alone decides.
A program may use at most 64 MiB of HBM per device.

```python
import math
import jax
import jax.numpy as jnp
from jax import lax

C = 1024
L = 8192
NF = 16384
K = 64


def with_ends(drawn, key, least, top_value):
    index_at = [jax.random.randint(jax.random.fold_in(key, axis), (), 0, length) for axis, length in enumerate(drawn.shape)]
    main_axis = drawn.shape.index(max(drawn.shape))
    beside = index_at[:main_axis] + [(index_at[main_axis] + 1) % drawn.shape[main_axis]] + index_at[main_axis + 1:]
    return drawn.at[tuple(index_at)].set(least).at[tuple(beside)].set(top_value)


def block_scale(stream_key, dims, shards, low, top_value):
    def one(position, blocks):
        steps = jax.random.uniform(jax.random.fold_in(jax.random.fold_in(stream_key, 6), position), (blocks,), jnp.float32, low / len(shards), top_value / len(shards))
        return jnp.repeat(jnp.exp(steps), dims[position] // blocks).reshape((-1,) + (1,) * (len(dims) - position - 1))

    factor_of = one(*shards[0])
    for cut in shards[1:]:
        factor_of = factor_of * one(*cut)
    return factor_of


def gaussian(rng, dims, deviation, limit, split=(), kind=jnp.bfloat16):
    array = deviation * jax.random.normal(rng, dims, jnp.float32)
    if split:
        array = array * block_scale(rng, dims, split, -0.22, 0.18)
    return jnp.clip(array, -limit, limit).astype(kind)


def setup_inputs(seed: int = 0, part: int = 0) -> dict:
    arg_keys = jax.random.split(jax.random.key(seed), 5)
    part_keys = jax.random.split(jax.random.fold_in(arg_keys[4], part), 5)
    return {
        "traces": gaussian(part_keys[0], (C, NF), 1.0, 6.0, ((1, 16),), jnp.float32),
        "templates": gaussian(arg_keys[1], (K, L), 1.0, 6.0, ((0, 16),), jnp.float32),
        "moveouts": with_ends(jax.random.randint(part_keys[2], (C,), 0, NF // 8), jax.random.fold_in(part_keys[2], 1), 0, (NF // 8) - 1).astype(jnp.int32),
        "masks": with_ends((jax.random.randint(part_keys[3], (K, C), 0, 4) < 3).astype(jnp.int32), jax.random.fold_in(part_keys[3], 1), 0, 1),
    }


def reference(traces, templates, moveouts, masks):
    length = traces.shape[1]
    spectra = jnp.fft.fft(traces, axis=1)
    freqs = jnp.arange(length).astype(jnp.int32)
    angle = 2.0 * math.pi / length * (moveouts.astype(jnp.int32)[:, None] * freqs[None, :] % length).astype(jnp.float32)
    moved = spectra * (jnp.cos(angle) + 1j * jnp.sin(angle))
    mask_float = masks.astype(jnp.float32)
    stacked_re = jnp.dot(mask_float, jnp.real(moved), precision=lax.Precision.HIGHEST, preferred_element_type=jnp.float32)
    stacked_im = jnp.dot(mask_float, jnp.imag(moved), precision=lax.Precision.HIGHEST, preferred_element_type=jnp.float32)
    template_spectra = jnp.fft.fft(templates, n=length, axis=1)
    product = (stacked_re + 1j * stacked_im) * jnp.conj(template_spectra)
    correlation = jnp.real(jnp.fft.ifft(product, axis=1))[:, :templates.shape[1]]
    energy = jnp.sqrt(lax.optimization_barrier(jnp.sum(templates * templates, axis=1)) + 1e-06)
    return correlation / (math.sqrt(traces.shape[0]) * energy[:, None])
```

```python
import functools
import math

import jax
import jax.numpy as jnp
import numpy as np
from jax import lax
from jax.experimental import pallas as pl
from jax.experimental.pallas import tpu as pltpu
from jax.sharding import PartitionSpec as P

f32, bf16 = jnp.float32, jnp.bfloat16
LANES = 128
REACH = 2048
COARSE = 4


def split(value):
    high = value.astype(bf16)
    return high, (value - high.astype(f32)).astype(bf16)


def split_table(table):
    high = table.astype(jnp.bfloat16)
    return high, (table - high.astype(np.float64)).astype(jnp.bfloat16)


def transform(rows, first_ref, forward_ref, cosine, sine):
    outer = cosine.shape[0]
    high, low = split(jnp.concatenate(rows, axis=1))
    first = jnp.dot(first_ref[...], jnp.concatenate([high, high, low], axis=0), preferred_element_type=f32)
    turned = []
    for r in range(len(rows)):
        re = first[:outer, r * LANES : (r + 1) * LANES]
        im = first[outer:, r * LANES : (r + 1) * LANES]
        turned.append(jnp.concatenate([re * cosine + im * sine, im * cosine - re * sine], axis=1))
    high, low = split(jnp.concatenate(turned, axis=0))
    return jnp.dot(jnp.concatenate([high, low, high], axis=1), forward_ref[...], preferred_element_type=f32)


def shift(traces_ref, late, terms, base, group, channels):
    rows = 16
    blocks = traces_ref.shape[1] // LANES
    here = pl.ds(pl.multiple_of(group * rows, rows), rows)
    delay = late[here, :]
    lane = lax.broadcasted_iota(jnp.int32, (rows, LANES), 1)
    inner = (delay & (LANES - 1)) + 1
    index = (lane - inner) & (LANES - 1)
    keep = lane >= inner
    turned = [
        jnp.take_along_axis(
            traces_ref[here, b * LANES : (b + 1) * LANES], index, axis=1, mode="promise_in_bounds"
        )
        for b in range(blocks)
    ]
    zero = jnp.zeros((rows, LANES), f32)
    moved = [
        jnp.where(keep, turned[b] if b < blocks else zero, turned[b - 1] if b > 0 else zero)
        for b in range(blocks + 1)
    ]
    hop = 1
    while hop < COARSE:
        chosen = ((delay // LANES) & hop) != 0
        moved = [
            jnp.where(
                chosen,
                moved[b - hop] if b >= hop else zero,
                moved[b] if b < len(moved) else zero,
            )
            for b in range(len(moved) + hop)
        ]
        hop *= 2
    for b in range(len(moved)):
        high, low = split(moved[b])
        column = slice(b * LANES, (b + 1) * LANES)
        terms[pl.ds(pl.multiple_of(base + group * rows, rows), rows), column] = high
        terms[pl.ds(pl.multiple_of(channels + base + group * rows, rows), rows), column] = low


def kernel(
    devices,
    channels,
    moveout_ref,
    moveouts_ref,
    traces_ref,
    mask_hbm,
    template_hbm,
    first_hbm,
    forward_hbm,
    back_hbm,
    last_hbm,
    twiddle_hbm,
    out_ref,
    mask_ref,
    template_ref,
    first_ref,
    forward_ref,
    back_ref,
    last_ref,
    twiddle_ref,
    late,
    terms,
    raw,
    part,
    arrived,
    merged,
    beside,
    joined,
    series,
    tail,
    load_sem,
    pair_send,
    pair_recv,
    beside_send,
    beside_recv,
    own_send,
    own_recv,
    sum_send,
    sum_recv,
):
    step = pl.program_id(0)
    steps = pl.num_programs(0)
    depth, width = traces_ref.shape
    each, lags = template_ref.shape
    pairs = devices // 2
    quads = devices // 4
    me = lax.axis_index("tm")
    core = lax.rem(me, 2)
    pair = me // 2
    quad = pair // 2
    side = lax.rem(pair, 2)
    partner = me + 1 - 2 * core
    blocks = width // LANES
    window = blocks + REACH // LANES
    outer = devices * blocks
    loads = [
        pltpu.make_async_copy(source, target, load_sem.at[i])
        for i, (source, target) in enumerate(
            (
                (mask_hbm, mask_ref),
                (template_hbm, template_ref),
                (first_hbm, first_ref),
                (forward_hbm, forward_ref),
                (twiddle_hbm, twiddle_ref),
                (back_hbm, back_ref),
                (last_hbm, last_ref),
            )
        )
    ]
    barrier = pltpu.get_barrier_semaphore()

    @pl.when(step == 0)
    def _():
        for load in loads:
            load.start()

        def greet(i, _):
            target = 2 * lax.rem(pair + i, pairs) + core
            pl.semaphore_signal(barrier, inc=1, device_id={"tm": target}, device_id_type=pl.DeviceIdType.MESH)
            return 0

        pl.semaphore_signal(barrier, inc=1, device_id={"tm": partner}, device_id_type=pl.DeviceIdType.MESH)
        lax.fori_loop(1, pairs, greet, 0)

    for piece in range(depth // LANES):
        row = (REACH - 1) - moveout_ref[:, piece * LANES : (piece + 1) * LANES]
        late[piece * LANES : (piece + 1) * LANES, :] = jnp.broadcast_to(row, (LANES, LANES)).T

    def four_groups(i, _):
        for k in range(4):
            shift(traces_ref, late, terms, step * depth, 4 * i + k, channels)
        return 0

    lax.fori_loop(0, depth // 64, four_groups, 0)

    def to_partner(g):
        return pltpu.make_async_remote_copy(
            src_ref=part.at[1 - core, g],
            dst_ref=arrived.at[g],
            send_sem=pair_send.at[g],
            recv_sem=pair_recv.at[g],
            device_id={"tm": partner},
            device_id_type=pl.DeviceIdType.MESH,
        )

    common, alone = REACH // LANES * each, 2 * blocks * each
    common_at = pl.multiple_of((1 - side) * alone, each)
    alone_at = pl.multiple_of(side * common, each)

    def to_beside(q):
        return pltpu.make_async_remote_copy(
            src_ref=merged.at[2 * q + 1 - side, pl.ds(common_at, common)],
            dst_ref=beside.at[q],
            send_sem=beside_send.at[q],
            recv_sem=beside_recv.at[q],
            device_id={"tm": 2 * (2 * quad + 1 - side) + core},
            device_id_type=pl.DeviceIdType.MESH,
        )

    def alone_copy(g, source_quad, source_side):
        return pltpu.make_async_remote_copy(
            src_ref=merged.at[g, pl.ds(alone_at, alone)],
            dst_ref=joined.at[
                source_quad, pl.ds(pl.multiple_of(source_side * (alone + common), each), alone)
            ],
            send_sem=own_send.at[g],
            recv_sem=own_recv.at[2 * source_quad + source_side],
            device_id={"tm": 2 * g + core},
            device_id_type=pl.DeviceIdType.MESH,
        )

    def sum_copy(q, source_quad):
        return pltpu.make_async_remote_copy(
            src_ref=merged.at[2 * q + side, pl.ds(common_at, common)],
            dst_ref=joined.at[source_quad, alone : alone + common],
            send_sem=sum_send.at[q],
            recv_sem=sum_recv.at[source_quad],
            device_id={"tm": 2 * (2 * q + side) + core},
            device_id_type=pl.DeviceIdType.MESH,
        )

    half = quads // 2

    def far(k):
        return (1 - quad // half) * half + lax.rem(quad + k, half)

    def near(k):
        return quad // half * half + lax.rem(quad + k, half)

    def in_order(body):
        def across(k, _):
            body(far(k))
            return 0

        def around(k, _):
            body(near(k))
            return 0

        lax.fori_loop(0, half, across, 0)
        lax.fori_loop(1, half, around, 0)

    @pl.when(step == steps - 1)
    def _():
        loads[0].wait()
        count = mask_ref.shape[0]
        coarse = ((REACH - 1) - moveouts_ref[...]) // (COARSE * LANES)
        chosen = [
            jnp.where(coarse == h, mask_ref[...], 0).astype(f32).astype(bf16)
            for h in range(REACH // LANES // COARSE)
        ]
        masks = jnp.concatenate(chosen, axis=0)
        double = jnp.concatenate([masks, masks], axis=1)
        fine = blocks + COARSE
        span = 2 if fine % 2 == 0 else 1
        for b in range(0, fine, span):
            column = slice(b * LANES, (b + span) * LANES)
            raw[:, column] = jnp.dot(double, terms[:, column], preferred_element_type=f32)

        def stacked(b):
            hops = [h for h in range(len(chosen)) if 0 <= b - COARSE * h < fine]
            return sum(
                raw[h * count : (h + 1) * count, (b - COARSE * h) * LANES : (b - COARSE * h + 1) * LANES]
                for h in hops
            )

        span = 2 if window % 2 == 0 else 1
        for b in range(0, window, span):
            added = [stacked(b + j) for j in range(span)]
            for owner in range(devices):
                part[owner % 2, owner // 2, b * each : (b + span) * each, :] = jnp.concatenate(
                    [value[owner * each : (owner + 1) * each] for value in added], axis=0
                )
        pl.semaphore_wait(barrier, pairs)

        def first_send(q):
            to_partner(2 * q + 1 - side).start()
            to_partner(2 * q + side).start()

        in_order(first_send)
        first_send(quad)
        rows, more = window * each, blocks * each

        def merge(g):
            to_partner(g).wait_recv()
            own, other = part[core, g], arrived[g]
            early = jnp.where(core == 0, own, other)
            later = jnp.where(core == 0, other, own)
            merged[g, 0:more] = early[:more]
            merged[g, more:rows] = early[more:] + later[: rows - more]
            merged[g, rows : rows + more] = later[rows - more :]

        def second_send(q):
            merge(2 * q + 1 - side)
            to_beside(q).start()
            alone_copy(2 * q + 1 - side, quad, side).start()
            merge(2 * q + side)
            alone_copy(2 * q + side, quad, side).start()

        in_order(second_send)
        merge(2 * quad + 1 - side)
        to_beside(quad).start()
        alone_copy(2 * quad + 1 - side, quad, side).start()
        merge(pair)

        for load in loads[1:]:
            load.wait()
        cosine, sine = twiddle_ref[0], twiddle_ref[1]
        values = template_ref[...]
        count = lags // LANES
        for b in range(count):
            series[b * each : (b + 1) * each, :] = values[:, b * LANES : (b + 1) * LANES]
        series[count * each :, :] = jnp.zeros(((outer - count) * each, LANES), f32)
        energy = jnp.sqrt(jnp.sum(values * values, axis=1, keepdims=True) + 1e-06)
        factor = 1.0 / (outer * LANES * math.sqrt(channels) * energy)

        def columns():
            return [series[pl.ds(k, outer, stride=each), :] for k in range(each)]

        templ = transform(columns(), first_ref, forward_ref, cosine, sine)

        def add_beside(q):
            to_beside(q).wait_recv()
            here = (2 * q + side, pl.ds(common_at, common))
            merged[here] = merged[here] + beside[q]

        def third_send(q):
            add_beside(q)
            sum_copy(q, quad).start()

        in_order(third_send)
        add_beside(quad)
        joined[quad, alone : alone + common] = merged[pair, pl.ds(common_at, common)]
        joined[quad, pl.ds(pl.multiple_of(side * (alone + common), each), alone)] = merged[
            pair, pl.ds(alone_at, alone)
        ]

        def finish(q):
            alone_copy(2 * q + 1 - side, q, 1 - side).wait()
            alone_copy(2 * q + side, q, side).wait()
            to_beside(q).wait_send()
            sum_copy(q, q).wait()

        in_order(finish)
        alone_copy(2 * quad + 1 - side, quad, 1 - side).wait()
        to_beside(quad).wait_send()

        def leave(g, _):
            to_partner(g).wait_send()
            return 0

        lax.fori_loop(0, pairs, leave, 0)
        series[...] = jnp.zeros(series.shape, f32)
        local = 2 * blocks
        wide = 2 * local + REACH // LANES
        for source in range(quads):
            for b in range(0, wide, local):
                taken = min(local, wide - b)
                block = (2 * source * local + b - REACH // LANES) % outer
                here = slice(block * each, (block + taken) * each)
                series[here, :] = series[here, :] + joined[source, b * each : (b + taken) * each, :]
        stack = transform(columns(), first_ref, forward_ref, cosine, sine)
        stack_re, stack_im = stack[:, :LANES], stack[:, LANES:]
        templ_re, templ_im = templ[:, :LANES], templ[:, LANES:]
        product = jnp.concatenate(
            [stack_re * templ_re + stack_im * templ_im, stack_im * templ_re - stack_re * templ_im], axis=1
        )
        high, low = split(product)
        back = jnp.dot(jnp.concatenate([high, low, high], axis=1), back_ref[...], preferred_element_type=f32)
        turned = []
        for k in range(each):
            re = back[k * outer : (k + 1) * outer, :LANES]
            im = back[k * outer : (k + 1) * outer, LANES:]
            turned.append(jnp.concatenate([re * cosine - im * sine, re * sine + im * cosine], axis=0))
        high, low = split(jnp.concatenate(turned, axis=1))
        final = jnp.dot(last_ref[...], jnp.concatenate([high, high, low], axis=0), preferred_element_type=f32)
        for k in range(each):
            tail[pl.ds(k, count, stride=each), :] = final[:, k * LANES : (k + 1) * LANES]
        for b in range(count):
            out_ref[:, b * LANES : (b + 1) * LANES] = tail[b * each : (b + 1) * each, :] * factor


def tables(length, lags):
    outer = length // LANES
    turn = 2.0 * math.pi
    ramp = np.arange(outer)[:, None] * np.arange(outer)[None, :] % outer * (turn / outer)
    wide = np.arange(LANES)[:, None] * np.arange(LANES)[None, :] % LANES * (turn / LANES)
    twist = np.arange(outer)[:, None] * np.arange(LANES)[None, :] % length * (turn / length)
    first = split_table(np.concatenate([np.cos(ramp), -np.sin(ramp)], axis=0))
    cosine, sine = np.cos(wide), np.sin(wide)
    forward = split_table(np.block([[cosine, -sine], [sine, cosine]]))
    back = split_table(np.block([[cosine, sine], [-sine, cosine]]))
    shown = ramp[: lags // LANES]
    last = split_table(np.concatenate([np.cos(shown), -np.sin(shown)], axis=1))
    return (
        np.concatenate([first[0], first[1], first[0]], axis=1),
        np.concatenate([forward[0], forward[0], forward[1]], axis=0),
        np.concatenate([back[0], back[0], back[1]], axis=0),
        np.concatenate([last[0], last[1], last[0]], axis=1),
        np.stack([np.cos(twist), np.sin(twist)]).astype(np.float32),
    )


def on_device(devices, traces, templates, moveouts, masks):
    channels, width = traces.shape
    each, lags = templates.shape
    blocks = width // LANES
    outer = devices * blocks
    window = blocks + REACH // LANES
    depth = math.gcd(channels, 256)
    pairs, quads = devices // 2, devices // 4
    loaded = [masks, templates, *[jnp.asarray(table) for table in tables(outer * LANES, lags)]]
    alone, common = 2 * blocks * each, REACH // LANES * each
    return pl.pallas_call(
        functools.partial(kernel, devices, channels),
        grid=(channels // depth,),
        in_specs=[
            pl.BlockSpec((1, depth), lambda i: (0, i)),
            pl.BlockSpec((1, channels), lambda i: (0, 0)),
            pl.BlockSpec((depth, width), lambda i: (i, 0)),
            *[pl.BlockSpec(memory_space=pl.ANY) for _ in loaded],
        ],
        out_specs=pl.BlockSpec((each, lags), lambda i: (0, 0)),
        out_shape=jax.ShapeDtypeStruct((each, lags), f32),
        scratch_shapes=[
            *[pltpu.VMEM(value.shape, value.dtype) for value in loaded],
            pltpu.VMEM((depth, LANES), jnp.int32),
            pltpu.VMEM((2 * channels, (blocks + COARSE) * LANES), bf16),
            pltpu.VMEM((REACH // LANES // COARSE * masks.shape[0], (blocks + COARSE) * LANES), f32),
            pltpu.VMEM((2, pairs, window * each, LANES), f32),
            pltpu.VMEM((pairs, window * each, LANES), f32),
            pltpu.VMEM((pairs, alone + common, LANES), f32),
            pltpu.VMEM((quads, common, LANES), f32),
            pltpu.VMEM((quads, 2 * alone + common, LANES), f32),
            pltpu.VMEM((outer * each, LANES), f32),
            pltpu.VMEM((lags // LANES * each, LANES), f32),
            pltpu.SemaphoreType.DMA((len(loaded),)),
            *[pltpu.SemaphoreType.DMA((count,)) for count in (pairs, pairs, quads, quads, pairs, pairs, quads, quads)],
        ],
        compiler_params=pltpu.CompilerParams(collective_id=0, has_side_effects=True),
        name="detect",
    )(moveouts[None, :], moveouts[None, :], traces, *loaded)


def solution(mesh):
    return jax.shard_map(
        functools.partial(on_device, mesh.shape["tm"]),
        mesh=mesh,
        in_specs=(P("grp", "tm"), P("tm", None), P("grp"), P(None, "grp")),
        out_specs=P("tm", "grp"),
        check_vma=False,
    )
```

```python
import functools
import math

import jax
import jax.numpy as jnp
import numpy as np
from jax import lax
from jax.experimental import pallas as pl
from jax.experimental.pallas import tpu as pltpu
from jax.sharding import PartitionSpec as P

f32, bf16 = jnp.float32, jnp.bfloat16
LANES = 128
REACH = 2048
COARSE = 4


def split(value):
    high = value.astype(bf16)
    return high, (value - high.astype(f32)).astype(bf16)


def split_table(table):
    high = table.astype(jnp.bfloat16)
    return high, (table - high.astype(np.float64)).astype(jnp.bfloat16)


def transform(rows, first_ref, forward_ref, cosine, sine):
    outer = cosine.shape[0]
    high, low = split(jnp.concatenate(rows, axis=1))
    first = jnp.dot(first_ref[...], jnp.concatenate([high, high, low], axis=0), preferred_element_type=f32)
    turned = []
    for r in range(len(rows)):
        re = first[:outer, r * LANES : (r + 1) * LANES]
        im = first[outer:, r * LANES : (r + 1) * LANES]
        turned.append(jnp.concatenate([re * cosine + im * sine, im * cosine - re * sine], axis=1))
    high, low = split(jnp.concatenate(turned, axis=0))
    return jnp.dot(jnp.concatenate([high, low, high], axis=1), forward_ref[...], preferred_element_type=f32)


def shift(traces, late, terms, row, target, depth):
    rows = 16
    blocks = traces.shape[1] // LANES
    here = slice(row, row + rows)
    delay = late[here, :]
    lane = lax.broadcasted_iota(jnp.int32, (rows, LANES), 1)
    inner = (delay & (LANES - 1)) + 1
    index = (lane - inner) & (LANES - 1)
    keep = lane >= inner
    turned = [
        jnp.take_along_axis(traces[here, b * LANES : (b + 1) * LANES], index, axis=1, mode="promise_in_bounds")
        for b in range(blocks)
    ]
    zero = jnp.zeros((rows, LANES), f32)
    moved = [
        jnp.where(keep, turned[b] if b < blocks else zero, turned[b - 1] if b > 0 else zero)
        for b in range(blocks + 1)
    ]
    hop = 1
    while hop < COARSE:
        chosen = ((delay // LANES) & hop) != 0
        moved = [
            jnp.where(
                chosen,
                moved[b - hop] if b >= hop else zero,
                moved[b] if b < len(moved) else zero,
            )
            for b in range(len(moved) + hop)
        ]
        hop *= 2
    for b in range(len(moved)):
        high, low = split(moved[b])
        column = slice(b * LANES, (b + 1) * LANES)
        terms[target : target + rows, column] = high
        terms[target + depth : target + depth + rows, column] = low


def kernel(
    devices,
    channels,
    moveouts_hbm,
    mask_hbm,
    traces_hbm,
    template_hbm,
    first_hbm,
    forward_hbm,
    back_hbm,
    last_hbm,
    twiddle_hbm,
    out_ref,
    moveouts_ref,
    mask_ref,
    template_ref,
    first_ref,
    forward_ref,
    back_ref,
    last_ref,
    twiddle_ref,
    traces,
    late,
    chosen,
    terms,
    raw,
    part,
    arrived,
    merged,
    beside,
    joined,
    series,
    tail,
    load_sem,
    trace_sem,
    pair_send,
    pair_recv,
    beside_send,
    beside_recv,
    own_send,
    own_recv,
    sum_send,
    sum_recv,
):
    width = traces.shape[1]
    depth = math.gcd(channels, 256)
    each, lags = template_ref.shape
    pairs = devices // 2
    quads = devices // 4
    me = lax.axis_index("tm")
    core = lax.rem(me, 2)
    pair = me // 2
    quad = pair // 2
    side = lax.rem(pair, 2)
    partner = me + 1 - 2 * core
    blocks = width // LANES
    window = blocks + REACH // LANES
    outer = devices * blocks
    loads = [
        pltpu.make_async_copy(source, target, load_sem.at[i])
        for i, (source, target) in enumerate(
            (
                (moveouts_hbm, moveouts_ref),
                (mask_hbm, mask_ref),
                (template_hbm, template_ref),
                (first_hbm, first_ref),
                (forward_hbm, forward_ref),
                (twiddle_hbm, twiddle_ref),
                (back_hbm, back_ref),
                (last_hbm, last_ref),
            )
        )
    ]
    barrier = pltpu.get_barrier_semaphore()

    fetches = [
        pltpu.make_async_copy(
            traces_hbm.at[p * LANES : (p + 1) * LANES], traces.at[p * LANES : (p + 1) * LANES], trace_sem.at[p]
        )
        for p in range(channels // LANES)
    ]
    for load in loads[:2] + fetches + loads[2:]:
        load.start()

    def greet(i, _):
        target = 2 * lax.rem(pair + i, pairs) + core
        pl.semaphore_signal(barrier, inc=1, device_id={"tm": target}, device_id_type=pl.DeviceIdType.MESH)
        return 0

    pl.semaphore_signal(barrier, inc=1, device_id={"tm": partner}, device_id_type=pl.DeviceIdType.MESH)
    lax.fori_loop(1, pairs, greet, 0)

    def to_partner(g):
        return pltpu.make_async_remote_copy(
            src_ref=part.at[1 - core, g],
            dst_ref=arrived.at[g],
            send_sem=pair_send.at[g],
            recv_sem=pair_recv.at[g],
            device_id={"tm": partner},
            device_id_type=pl.DeviceIdType.MESH,
        )

    common, alone = REACH // LANES * each, 2 * blocks * each
    common_at = pl.multiple_of((1 - side) * alone, each)
    alone_at = pl.multiple_of(side * common, each)

    def to_beside(q):
        return pltpu.make_async_remote_copy(
            src_ref=merged.at[2 * q + 1 - side, pl.ds(common_at, common)],
            dst_ref=beside.at[q],
            send_sem=beside_send.at[q],
            recv_sem=beside_recv.at[q],
            device_id={"tm": 2 * (2 * quad + 1 - side) + core},
            device_id_type=pl.DeviceIdType.MESH,
        )

    def alone_copy(g, source_quad, source_side):
        return pltpu.make_async_remote_copy(
            src_ref=merged.at[g, pl.ds(alone_at, alone)],
            dst_ref=joined.at[
                source_quad, pl.ds(pl.multiple_of(source_side * (alone + common), each), alone)
            ],
            send_sem=own_send.at[g],
            recv_sem=own_recv.at[2 * source_quad + source_side],
            device_id={"tm": 2 * g + core},
            device_id_type=pl.DeviceIdType.MESH,
        )

    def sum_copy(q, source_quad):
        return pltpu.make_async_remote_copy(
            src_ref=merged.at[2 * q + side, pl.ds(common_at, common)],
            dst_ref=joined.at[source_quad, alone : alone + common],
            send_sem=sum_send.at[q],
            recv_sem=sum_recv.at[source_quad],
            device_id={"tm": 2 * (2 * q + side) + core},
            device_id_type=pl.DeviceIdType.MESH,
        )

    def in_order(body):
        def visit(q, _):
            body(q)
            return 0

        lax.fori_loop(0, quad, visit, 0)
        lax.fori_loop(quad + 1, quads, visit, 0)

    loads[0].wait()
    for p in range(channels // LANES):
        row = (REACH - 1) - moveouts_ref[:, p * LANES : (p + 1) * LANES]
        late[p * LANES : (p + 1) * LANES, :] = jnp.broadcast_to(row, (LANES, LANES)).T
    loads[1].wait()
    count = mask_ref.shape[0]
    coarse = ((REACH - 1) - moveouts_ref[...]) // (COARSE * LANES)
    hops = REACH // LANES // COARSE
    for h in range(hops):
        chosen[h * count : (h + 1) * count, :] = (
            jnp.where(coarse == h, mask_ref[...], 0).astype(f32).astype(bf16)
        )
    fine = blocks + COARSE
    span = 2 if fine % 2 == 0 else 1

    def combine(c):
        one = chosen[:, c * depth : (c + 1) * depth]
        double = jnp.concatenate([one, one], axis=1)
        for b in range(0, fine, span):
            column = slice(b * LANES, (b + span) * LANES)
            value = jnp.dot(
                double, terms[2 * c * depth : 2 * (c + 1) * depth, column], preferred_element_type=f32
            )
            raw[:, column] = value if c == 0 else raw[:, column] + value

    for c in range(channels // depth):
        for p in range(c * depth // LANES, (c + 1) * depth // LANES):
            fetches[p].wait()
        for row in range(0, depth, 16):
            shift(traces, late, terms, c * depth + row, 2 * c * depth + row, depth)
        if c > 0:
            combine(c - 1)
    combine(channels // depth - 1)

    def stacked(b):
        found = [h for h in range(hops) if 0 <= b - COARSE * h < fine]
        return sum(
            raw[h * count : (h + 1) * count, (b - COARSE * h) * LANES : (b - COARSE * h + 1) * LANES]
            for h in found
        )

    span = 2 if window % 2 == 0 else 1
    for b in range(0, window, span):
        added = [stacked(b + j) for j in range(span)]
        for owner in range(devices):
            part[owner % 2, owner // 2, b * each : (b + span) * each, :] = jnp.concatenate(
                [value[owner * each : (owner + 1) * each] for value in added], axis=0
            )
    pl.semaphore_wait(barrier, pairs)

    def first_send(q):
        to_partner(2 * q + 1 - side).start()
        to_partner(2 * q + side).start()

    in_order(first_send)
    first_send(quad)
    rows, more = window * each, blocks * each

    def merge(g):
        to_partner(g).wait_recv()
        own, other = part[core, g], arrived[g]
        early = jnp.where(core == 0, own, other)
        later = jnp.where(core == 0, other, own)
        merged[g, 0:more] = early[:more]
        merged[g, more:rows] = early[more:] + later[: rows - more]
        merged[g, rows : rows + more] = later[rows - more :]

    def second_send(q):
        merge(2 * q + 1 - side)
        to_beside(q).start()
        alone_copy(2 * q + 1 - side, quad, side).start()
        merge(2 * q + side)
        alone_copy(2 * q + side, quad, side).start()

    in_order(second_send)
    merge(2 * quad + 1 - side)
    to_beside(quad).start()
    alone_copy(2 * quad + 1 - side, quad, side).start()
    merge(pair)

    for load in loads[2:]:
        load.wait()
    cosine, sine = twiddle_ref[0], twiddle_ref[1]
    values = template_ref[...]
    count = lags // LANES
    for b in range(count):
        series[b * each : (b + 1) * each, :] = values[:, b * LANES : (b + 1) * LANES]
    series[count * each :, :] = jnp.zeros(((outer - count) * each, LANES), f32)
    energy = jnp.sqrt(jnp.sum(values * values, axis=1, keepdims=True) + 1e-06)
    factor = 1.0 / (outer * LANES * math.sqrt(channels) * energy)

    def columns():
        return [series[pl.ds(k, outer, stride=each), :] for k in range(each)]

    templ = transform(columns(), first_ref, forward_ref, cosine, sine)

    def add_beside(q):
        to_beside(q).wait_recv()
        here = (2 * q + side, pl.ds(common_at, common))
        merged[here] = merged[here] + beside[q]

    def third_send(q):
        add_beside(q)
        sum_copy(q, quad).start()

    in_order(third_send)
    add_beside(quad)
    joined[quad, alone : alone + common] = merged[pair, pl.ds(common_at, common)]
    joined[quad, pl.ds(pl.multiple_of(side * (alone + common), each), alone)] = merged[
        pair, pl.ds(alone_at, alone)
    ]

    def finish(q):
        alone_copy(2 * q + 1 - side, q, 1 - side).wait()
        alone_copy(2 * q + side, q, side).wait()
        to_beside(q).wait_send()
        sum_copy(q, q).wait()

    in_order(finish)
    alone_copy(2 * quad + 1 - side, quad, 1 - side).wait()
    to_beside(quad).wait_send()

    def leave(g, _):
        to_partner(g).wait_send()
        return 0

    lax.fori_loop(0, pairs, leave, 0)
    series[...] = jnp.zeros(series.shape, f32)
    local = 2 * blocks
    wide = 2 * local + REACH // LANES
    for source in range(quads):
        for b in range(0, wide, local):
            taken = min(local, wide - b)
            block = (2 * source * local + b - REACH // LANES) % outer
            here = slice(block * each, (block + taken) * each)
            series[here, :] = series[here, :] + joined[source, b * each : (b + taken) * each, :]
    stack = transform(columns(), first_ref, forward_ref, cosine, sine)
    stack_re, stack_im = stack[:, :LANES], stack[:, LANES:]
    templ_re, templ_im = templ[:, :LANES], templ[:, LANES:]
    product = jnp.concatenate(
        [stack_re * templ_re + stack_im * templ_im, stack_im * templ_re - stack_re * templ_im], axis=1
    )
    high, low = split(product)
    back = jnp.dot(jnp.concatenate([high, low, high], axis=1), back_ref[...], preferred_element_type=f32)
    turned = []
    for k in range(each):
        re = back[k * outer : (k + 1) * outer, :LANES]
        im = back[k * outer : (k + 1) * outer, LANES:]
        turned.append(jnp.concatenate([re * cosine - im * sine, re * sine + im * cosine], axis=0))
    high, low = split(jnp.concatenate(turned, axis=1))
    final = jnp.dot(last_ref[...], jnp.concatenate([high, high, low], axis=0), preferred_element_type=f32)
    for k in range(each):
        tail[pl.ds(k, count, stride=each), :] = final[:, k * LANES : (k + 1) * LANES]
    for b in range(count):
        out_ref[:, b * LANES : (b + 1) * LANES] = tail[b * each : (b + 1) * each, :] * factor


def tables(length, lags):
    outer = length // LANES
    turn = 2.0 * math.pi
    ramp = np.arange(outer)[:, None] * np.arange(outer)[None, :] % outer * (turn / outer)
    wide = np.arange(LANES)[:, None] * np.arange(LANES)[None, :] % LANES * (turn / LANES)
    twist = np.arange(outer)[:, None] * np.arange(LANES)[None, :] % length * (turn / length)
    first = split_table(np.concatenate([np.cos(ramp), -np.sin(ramp)], axis=0))
    cosine, sine = np.cos(wide), np.sin(wide)
    forward = split_table(np.block([[cosine, -sine], [sine, cosine]]))
    back = split_table(np.block([[cosine, sine], [-sine, cosine]]))
    shown = ramp[: lags // LANES]
    last = split_table(np.concatenate([np.cos(shown), -np.sin(shown)], axis=1))
    return (
        np.concatenate([first[0], first[1], first[0]], axis=1),
        np.concatenate([forward[0], forward[0], forward[1]], axis=0),
        np.concatenate([back[0], back[0], back[1]], axis=0),
        np.concatenate([last[0], last[1], last[0]], axis=1),
        np.stack([np.cos(twist), np.sin(twist)]).astype(np.float32),
    )


def on_device(devices, traces, templates, moveouts, masks):
    channels, width = traces.shape
    each, lags = templates.shape
    blocks = width // LANES
    outer = devices * blocks
    window = blocks + REACH // LANES
    pairs, quads = devices // 2, devices // 4
    loaded = [moveouts[None, :], masks, templates, *[jnp.asarray(table) for table in tables(outer * LANES, lags)]]
    alone, common = 2 * blocks * each, REACH // LANES * each
    return pl.pallas_call(
        functools.partial(kernel, devices, channels),
        in_specs=[pl.BlockSpec(memory_space=pl.ANY) for _ in range(len(loaded) + 1)],
        out_specs=pl.BlockSpec(memory_space=pltpu.VMEM),
        out_shape=pltpu.VMEM((each, lags), f32),
        scratch_shapes=[
            *[pltpu.VMEM(value.shape, value.dtype) for value in loaded],
            pltpu.VMEM((channels, width), f32),
            pltpu.VMEM((channels, LANES), jnp.int32),
            pltpu.VMEM((REACH // LANES // COARSE * masks.shape[0], channels), bf16),
            pltpu.VMEM((2 * channels, (blocks + COARSE) * LANES), bf16),
            pltpu.VMEM((REACH // LANES // COARSE * masks.shape[0], (blocks + COARSE) * LANES), f32),
            pltpu.VMEM((2, pairs, window * each, LANES), f32),
            pltpu.VMEM((pairs, window * each, LANES), f32),
            pltpu.VMEM((pairs, alone + common, LANES), f32),
            pltpu.VMEM((quads, common, LANES), f32),
            pltpu.VMEM((quads, 2 * alone + common, LANES), f32),
            pltpu.VMEM((outer * each, LANES), f32),
            pltpu.VMEM((lags // LANES * each, LANES), f32),
            pltpu.SemaphoreType.DMA((len(loaded),)),
            pltpu.SemaphoreType.DMA((channels // LANES,)),
            *[pltpu.SemaphoreType.DMA((count,)) for count in (pairs, pairs, quads, quads, pairs, pairs, quads, quads)],
        ],
        compiler_params=pltpu.CompilerParams(collective_id=0, has_side_effects=True),
        name="detect",
    )(*loaded[:2], traces, *loaded[2:])


def solution(mesh):
    return jax.shard_map(
        functools.partial(on_device, mesh.shape["tm"]),
        mesh=mesh,
        in_specs=(P("grp", "tm"), P("tm", None), P("grp"), P(None, "grp")),
        out_specs=P("tm", "grp"),
        check_vma=False,
    )
```

```python
import functools
import math

import jax
import jax.numpy as jnp
import numpy as np
from jax import lax
from jax.experimental import pallas as pl
from jax.experimental.pallas import tpu as pltpu
from jax.sharding import PartitionSpec as P

f32, bf16 = jnp.float32, jnp.bfloat16
LANES = 128
REACH = 2048
COARSE = 4


def split(value):
    high = value.astype(bf16)
    return high, (value - high.astype(f32)).astype(bf16)


def split_table(table):
    high = table.astype(jnp.bfloat16)
    return high, (table - high.astype(np.float64)).astype(jnp.bfloat16)


def transform(rows, first_ref, forward_ref, cosine, sine):
    outer = cosine.shape[0]
    high, low = split(jnp.concatenate(rows, axis=1))
    first = jnp.dot(first_ref[...], jnp.concatenate([high, high, low], axis=0), preferred_element_type=f32)
    turned = []
    for r in range(len(rows)):
        re = first[:outer, r * LANES : (r + 1) * LANES]
        im = first[outer:, r * LANES : (r + 1) * LANES]
        turned.append(jnp.concatenate([re * cosine + im * sine, im * cosine - re * sine], axis=1))
    high, low = split(jnp.concatenate(turned, axis=0))
    return jnp.dot(jnp.concatenate([high, low, high], axis=1), forward_ref[...], preferred_element_type=f32)


def shift(traces, late, terms, row, target, depth):
    rows = 8
    blocks = traces.shape[1] // LANES
    here = slice(row, row + rows)
    delay = late[here, :]
    lane = lax.broadcasted_iota(jnp.int32, (rows, LANES), 1)
    inner = (delay & (LANES - 1)) + 1
    index = (lane - inner) & (LANES - 1)
    keep = lane >= inner
    turned = [
        jnp.take_along_axis(traces[here, b * LANES : (b + 1) * LANES], index, axis=1, mode="promise_in_bounds")
        for b in range(blocks)
    ]
    zero = jnp.zeros((rows, LANES), f32)
    moved = [
        jnp.where(keep, turned[b] if b < blocks else zero, turned[b - 1] if b > 0 else zero)
        for b in range(blocks + 1)
    ]
    hop = 1
    while hop < COARSE:
        chosen = ((delay // LANES) & hop) != 0
        moved = [
            jnp.where(
                chosen,
                moved[b - hop] if b >= hop else zero,
                moved[b] if b < len(moved) else zero,
            )
            for b in range(len(moved) + hop)
        ]
        hop *= 2
    span = 2 if len(moved) % 2 == 0 else 1
    for b in range(0, len(moved), span):
        high, low = split(jnp.concatenate(moved[b : b + span], axis=1))
        column = slice(b * LANES, (b + span) * LANES)
        terms[target : target + rows, column] = high
        terms[target + depth : target + depth + rows, column] = low


def kernel(
    devices,
    channels,
    moveouts_hbm,
    mask_hbm,
    traces_hbm,
    template_hbm,
    first_hbm,
    forward_hbm,
    back_hbm,
    last_hbm,
    twiddle_hbm,
    out_ref,
    moveouts_ref,
    mask_ref,
    template_ref,
    first_ref,
    forward_ref,
    back_ref,
    last_ref,
    twiddle_ref,
    traces,
    late,
    chosen,
    terms,
    raw,
    part,
    arrived,
    merged,
    beside,
    joined,
    series,
    tail,
    load_sem,
    trace_sem,
    pair_send,
    pair_recv,
    beside_send,
    beside_recv,
    own_send,
    own_recv,
    sum_send,
    sum_recv,
):
    width = traces.shape[1]
    depth = math.gcd(channels, 256)
    each, lags = template_ref.shape
    pairs = devices // 2
    quads = devices // 4
    me = lax.axis_index("tm")
    core = lax.rem(me, 2)
    pair = me // 2
    quad = pair // 2
    side = lax.rem(pair, 2)
    partner = me + 1 - 2 * core
    blocks = width // LANES
    window = blocks + REACH // LANES
    outer = devices * blocks
    loads = [
        pltpu.make_async_copy(source, target, load_sem.at[i])
        for i, (source, target) in enumerate(
            (
                (moveouts_hbm, moveouts_ref),
                (mask_hbm, mask_ref),
                (template_hbm, template_ref),
                (first_hbm, first_ref),
                (forward_hbm, forward_ref),
                (twiddle_hbm, twiddle_ref),
                (back_hbm, back_ref),
                (last_hbm, last_ref),
            )
        )
    ]
    barrier = pltpu.get_barrier_semaphore()

    fetches = [
        pltpu.make_async_copy(
            traces_hbm.at[p * LANES : (p + 1) * LANES], traces.at[p * LANES : (p + 1) * LANES], trace_sem.at[p]
        )
        for p in range(channels // LANES)
    ]
    first_rows = depth // LANES
    for load in loads[:1] + fetches[:first_rows] + loads[1:2] + fetches[first_rows:] + loads[2:]:
        load.start()

    def greet(i, _):
        target = 2 * lax.rem(pair + i, pairs) + core
        pl.semaphore_signal(barrier, inc=1, device_id={"tm": target}, device_id_type=pl.DeviceIdType.MESH)
        return 0

    pl.semaphore_signal(barrier, inc=1, device_id={"tm": partner}, device_id_type=pl.DeviceIdType.MESH)
    lax.fori_loop(1, pairs, greet, 0)

    def to_partner(g):
        return pltpu.make_async_remote_copy(
            src_ref=part.at[1 - core, g],
            dst_ref=arrived.at[g],
            send_sem=pair_send.at[g],
            recv_sem=pair_recv.at[g],
            device_id={"tm": partner},
            device_id_type=pl.DeviceIdType.MESH,
        )

    common, alone = REACH // LANES * each, 2 * blocks * each
    common_at = pl.multiple_of((1 - side) * alone, each)
    alone_at = pl.multiple_of(side * common, each)

    def to_beside(q):
        return pltpu.make_async_remote_copy(
            src_ref=merged.at[2 * q + 1 - side, pl.ds(common_at, common)],
            dst_ref=beside.at[q],
            send_sem=beside_send.at[q],
            recv_sem=beside_recv.at[q],
            device_id={"tm": 2 * (2 * quad + 1 - side) + core},
            device_id_type=pl.DeviceIdType.MESH,
        )

    def alone_copy(g, source_quad, source_side):
        return pltpu.make_async_remote_copy(
            src_ref=merged.at[g, pl.ds(alone_at, alone)],
            dst_ref=joined.at[
                source_quad, pl.ds(pl.multiple_of(source_side * (alone + common), each), alone)
            ],
            send_sem=own_send.at[g],
            recv_sem=own_recv.at[2 * source_quad + source_side],
            device_id={"tm": 2 * g + core},
            device_id_type=pl.DeviceIdType.MESH,
        )

    def sum_copy(q, source_quad):
        return pltpu.make_async_remote_copy(
            src_ref=merged.at[2 * q + side, pl.ds(common_at, common)],
            dst_ref=joined.at[source_quad, alone : alone + common],
            send_sem=sum_send.at[q],
            recv_sem=sum_recv.at[source_quad],
            device_id={"tm": 2 * (2 * q + side) + core},
            device_id_type=pl.DeviceIdType.MESH,
        )

    def in_order(body):
        def visit(q, _):
            body(q)
            return 0

        lax.fori_loop(0, quad, visit, 0)
        lax.fori_loop(quad + 1, quads, visit, 0)

    loads[0].wait()
    for p in range(channels // LANES):
        row = (REACH - 1) - moveouts_ref[:, p * LANES : (p + 1) * LANES]
        late[p * LANES : (p + 1) * LANES, :] = jnp.broadcast_to(row, (LANES, LANES)).T
    count = mask_ref.shape[0]
    hops = REACH // LANES // COARSE

    def choose():
        loads[1].wait()
        coarse = ((REACH - 1) - moveouts_ref[...]) // (COARSE * LANES)
        for h in range(hops):
            chosen[h * count : (h + 1) * count, :] = (
                jnp.where(coarse == h, mask_ref[...], 0).astype(f32).astype(bf16)
            )

    fine = blocks + COARSE
    span = 2 if fine % 2 == 0 else 1

    def combine(c):
        one = chosen[:, c * depth : (c + 1) * depth]
        double = jnp.concatenate([one, one], axis=1)
        for b in range(0, fine, span):
            column = slice(b * LANES, (b + span) * LANES)
            value = jnp.dot(
                double, terms[2 * c * depth : 2 * (c + 1) * depth, column], preferred_element_type=f32
            )
            raw[:, column] = value if c == 0 else raw[:, column] + value

    for c in range(channels // depth):
        for p in range(c * depth // LANES, (c + 1) * depth // LANES):
            fetches[p].wait()
        if c == 1:
            choose()
        for row in range(0, depth, 8):
            shift(traces, late, terms, c * depth + row, 2 * c * depth + row, depth)
        if c > 0:
            combine(c - 1)
    if channels == depth:
        choose()
    combine(channels // depth - 1)

    def stacked(b):
        found = [h for h in range(hops) if 0 <= b - COARSE * h < fine]
        return sum(
            raw[h * count : (h + 1) * count, (b - COARSE * h) * LANES : (b - COARSE * h + 1) * LANES]
            for h in found
        )

    span = 2 if window % 2 == 0 else 1
    for b in range(0, window, span):
        added = [stacked(b + j) for j in range(span)]
        for owner in range(devices):
            part[owner % 2, owner // 2, b * each : (b + span) * each, :] = jnp.concatenate(
                [value[owner * each : (owner + 1) * each] for value in added], axis=0
            )
    pl.semaphore_wait(barrier, pairs)

    def first_send(q):
        to_partner(2 * q + 1 - side).start()
        to_partner(2 * q + side).start()

    in_order(first_send)
    first_send(quad)
    rows, more = window * each, blocks * each

    def merge(g):
        to_partner(g).wait_recv()
        own, other = part[core, g], arrived[g]
        early = jnp.where(core == 0, own, other)
        later = jnp.where(core == 0, other, own)
        merged[g, 0:more] = early[:more]
        merged[g, more:rows] = early[more:] + later[: rows - more]
        merged[g, rows : rows + more] = later[rows - more :]

    def alone_send(q):
        alone_copy(2 * q + 1 - side, quad, side).start()
        alone_copy(2 * q + side, quad, side).start()

    def second_send(q):
        merge(2 * q + 1 - side)
        to_beside(q).start()
        merge(2 * q + side)

        @pl.when((q == 0) | (q > quad))
        def _():
            alone_copy(2 * q + side, quad, side).start()

        @pl.when(q == 0)
        def _():
            alone_copy(2 * q + 1 - side, quad, side).start()

    in_order(second_send)
    merge(2 * quad + 1 - side)
    to_beside(quad).start()
    alone_copy(2 * quad + 1 - side, quad, side).start()
    merge(pair)

    for load in loads[2:]:
        load.wait()
    cosine, sine = twiddle_ref[0], twiddle_ref[1]
    values = template_ref[...]
    count = lags // LANES
    for b in range(count):
        series[b * each : (b + 1) * each, :] = values[:, b * LANES : (b + 1) * LANES]
    series[count * each :, :] = jnp.zeros(((outer - count) * each, LANES), f32)
    energy = jnp.sqrt(jnp.sum(values * values, axis=1, keepdims=True) + 1e-06)
    factor = 1.0 / (outer * LANES * math.sqrt(channels) * energy)

    def columns():
        return [series[pl.ds(k, outer, stride=each), :] for k in range(each)]

    templ = transform(columns(), first_ref, forward_ref, cosine, sine)

    def add_beside(q):
        to_beside(q).wait_recv()
        here = (2 * q + side, pl.ds(common_at, common))
        merged[here] = merged[here] + beside[q]

    def third_send(q):
        add_beside(q)
        sum_copy(q, quad).start()

        @pl.when(q + 1 < quad)
        def _():
            alone_send(q + 1)

    in_order(third_send)

    def fourth_send(q, _):
        alone_copy(2 * q + 1 - side, quad, side).start()
        return 0

    lax.fori_loop(quad + 1, quads, fourth_send, 0)
    add_beside(quad)
    joined[quad, alone : alone + common] = merged[pair, pl.ds(common_at, common)]
    joined[quad, pl.ds(pl.multiple_of(side * (alone + common), each), alone)] = merged[
        pair, pl.ds(alone_at, alone)
    ]

    def finish(q):
        alone_copy(2 * q + 1 - side, q, 1 - side).wait()
        alone_copy(2 * q + side, q, side).wait()
        to_beside(q).wait_send()
        sum_copy(q, q).wait()

    in_order(finish)
    alone_copy(2 * quad + 1 - side, quad, 1 - side).wait()
    to_beside(quad).wait_send()

    def leave(g, _):
        to_partner(g).wait_send()
        return 0

    lax.fori_loop(0, pairs, leave, 0)
    series[...] = jnp.zeros(series.shape, f32)
    local = 2 * blocks
    wide = 2 * local + REACH // LANES
    for source in range(quads):
        for b in range(0, wide, local):
            taken = min(local, wide - b)
            block = (2 * source * local + b - REACH // LANES) % outer
            here = slice(block * each, (block + taken) * each)
            series[here, :] = series[here, :] + joined[source, b * each : (b + taken) * each, :]
    stack = transform(columns(), first_ref, forward_ref, cosine, sine)
    stack_re, stack_im = stack[:, :LANES], stack[:, LANES:]
    templ_re, templ_im = templ[:, :LANES], templ[:, LANES:]
    product = jnp.concatenate(
        [stack_re * templ_re + stack_im * templ_im, stack_im * templ_re - stack_re * templ_im], axis=1
    )
    high, low = split(product)
    back = jnp.dot(jnp.concatenate([high, low, high], axis=1), back_ref[...], preferred_element_type=f32)
    turned = []
    for k in range(each):
        re = back[k * outer : (k + 1) * outer, :LANES]
        im = back[k * outer : (k + 1) * outer, LANES:]
        turned.append(jnp.concatenate([re * cosine - im * sine, re * sine + im * cosine], axis=0))
    high, low = split(jnp.concatenate(turned, axis=1))
    final = jnp.dot(last_ref[...], jnp.concatenate([high, high, low], axis=0), preferred_element_type=f32)
    for k in range(each):
        tail[pl.ds(k, count, stride=each), :] = final[:, k * LANES : (k + 1) * LANES]
    for b in range(count):
        out_ref[:, b * LANES : (b + 1) * LANES] = tail[b * each : (b + 1) * each, :] * factor


def tables(length, lags):
    outer = length // LANES
    turn = 2.0 * math.pi
    ramp = np.arange(outer)[:, None] * np.arange(outer)[None, :] % outer * (turn / outer)
    wide = np.arange(LANES)[:, None] * np.arange(LANES)[None, :] % LANES * (turn / LANES)
    twist = np.arange(outer)[:, None] * np.arange(LANES)[None, :] % length * (turn / length)
    first = split_table(np.concatenate([np.cos(ramp), -np.sin(ramp)], axis=0))
    cosine, sine = np.cos(wide), np.sin(wide)
    forward = split_table(np.block([[cosine, -sine], [sine, cosine]]))
    back = split_table(np.block([[cosine, sine], [-sine, cosine]]))
    shown = ramp[: lags // LANES]
    last = split_table(np.concatenate([np.cos(shown), -np.sin(shown)], axis=1))
    return (
        np.concatenate([first[0], first[1], first[0]], axis=1),
        np.concatenate([forward[0], forward[0], forward[1]], axis=0),
        np.concatenate([back[0], back[0], back[1]], axis=0),
        np.concatenate([last[0], last[1], last[0]], axis=1),
        np.stack([np.cos(twist), np.sin(twist)]).astype(np.float32),
    )


def on_device(devices, traces, templates, moveouts, masks):
    channels, width = traces.shape
    each, lags = templates.shape
    blocks = width // LANES
    outer = devices * blocks
    window = blocks + REACH // LANES
    pairs, quads = devices // 2, devices // 4
    loaded = [moveouts[None, :], masks, templates, *[jnp.asarray(table) for table in tables(outer * LANES, lags)]]
    alone, common = 2 * blocks * each, REACH // LANES * each
    return pl.pallas_call(
        functools.partial(kernel, devices, channels),
        in_specs=[pl.BlockSpec(memory_space=pl.ANY) for _ in range(len(loaded) + 1)],
        out_specs=pl.BlockSpec(memory_space=pltpu.VMEM),
        out_shape=pltpu.VMEM((each, lags), f32),
        scratch_shapes=[
            *[pltpu.VMEM(value.shape, value.dtype) for value in loaded],
            pltpu.VMEM((channels, width), f32),
            pltpu.VMEM((channels, LANES), jnp.int32),
            pltpu.VMEM((REACH // LANES // COARSE * masks.shape[0], channels), bf16),
            pltpu.VMEM((2 * channels, (blocks + COARSE) * LANES), bf16),
            pltpu.VMEM((REACH // LANES // COARSE * masks.shape[0], (blocks + COARSE) * LANES), f32),
            pltpu.VMEM((2, pairs, window * each, LANES), f32),
            pltpu.VMEM((pairs, window * each, LANES), f32),
            pltpu.VMEM((pairs, alone + common, LANES), f32),
            pltpu.VMEM((quads, common, LANES), f32),
            pltpu.VMEM((quads, 2 * alone + common, LANES), f32),
            pltpu.VMEM((outer * each, LANES), f32),
            pltpu.VMEM((lags // LANES * each, LANES), f32),
            pltpu.SemaphoreType.DMA((len(loaded),)),
            pltpu.SemaphoreType.DMA((channels // LANES,)),
            *[pltpu.SemaphoreType.DMA((count,)) for count in (pairs, pairs, quads, quads, pairs, pairs, quads, quads)],
        ],
        compiler_params=pltpu.CompilerParams(collective_id=0, has_side_effects=True),
        name="detect",
    )(*loaded[:2], traces, *loaded[2:])


def solution(mesh):
    return jax.shard_map(
        functools.partial(on_device, mesh.shape["tm"]),
        mesh=mesh,
        in_specs=(P("grp", "tm"), P("tm", None), P("grp"), P(None, "grp")),
        out_specs=P("tm", "grp"),
        check_vma=False,
    )
```

```python
import functools
import math

import jax
import jax.numpy as jnp
import numpy as np
from jax import lax
from jax.experimental import pallas as pl
from jax.experimental.pallas import tpu as pltpu
from jax.sharding import PartitionSpec as P

f32, bf16 = jnp.float32, jnp.bfloat16
LANES = 128
REACH = 2048
COARSE = 4


def split(value):
    high = value.astype(bf16)
    return high, (value - high.astype(f32)).astype(bf16)


def split_table(table):
    high = table.astype(jnp.bfloat16)
    return high, (table - high.astype(np.float64)).astype(jnp.bfloat16)


def transform(rows, first_ref, forward_ref, cosine, sine):
    outer = cosine.shape[0]
    high, low = split(jnp.concatenate(rows, axis=1))
    first = jnp.dot(first_ref[...], jnp.concatenate([high, high, low], axis=0), preferred_element_type=f32)
    turned = []
    for r in range(len(rows)):
        re = first[:outer, r * LANES : (r + 1) * LANES]
        im = first[outer:, r * LANES : (r + 1) * LANES]
        turned.append(jnp.concatenate([re * cosine + im * sine, im * cosine - re * sine], axis=1))
    high, low = split(jnp.concatenate(turned, axis=0))
    return jnp.dot(jnp.concatenate([high, low, high], axis=1), forward_ref[...], preferred_element_type=f32)


def shift(traces, late, terms, row, target, depth):
    rows = 8
    blocks = traces.shape[1] // LANES
    here = slice(row, row + rows)
    delay = late[here, :]
    lane = lax.broadcasted_iota(jnp.int32, (rows, LANES), 1)
    inner = (delay & (LANES - 1)) + 1
    index = (lane - inner) & (LANES - 1)
    keep = lane >= inner
    turned = [
        jnp.take_along_axis(traces[here, b * LANES : (b + 1) * LANES], index, axis=1, mode="promise_in_bounds")
        for b in range(blocks)
    ]
    zero = jnp.zeros((rows, LANES), f32)
    moved = [
        jnp.where(keep, turned[b] if b < blocks else zero, turned[b - 1] if b > 0 else zero)
        for b in range(blocks + 1)
    ]
    hop = 1
    while hop < COARSE:
        chosen = ((delay // LANES) & hop) != 0
        moved = [
            jnp.where(
                chosen,
                moved[b - hop] if b >= hop else zero,
                moved[b] if b < len(moved) else zero,
            )
            for b in range(len(moved) + hop)
        ]
        hop *= 2
    span = 2 if len(moved) % 2 == 0 else 1
    for b in range(0, len(moved), span):
        high, low = split(jnp.concatenate(moved[b : b + span], axis=1))
        column = slice(b * LANES, (b + span) * LANES)
        terms[target : target + rows, column] = high
        terms[target + depth : target + depth + rows, column] = low


def kernel(
    devices,
    channels,
    moveouts_hbm,
    mask_hbm,
    traces_hbm,
    template_hbm,
    first_hbm,
    forward_hbm,
    back_hbm,
    last_hbm,
    twiddle_hbm,
    out_ref,
    moveouts_ref,
    mask_ref,
    template_ref,
    first_ref,
    forward_ref,
    back_ref,
    last_ref,
    twiddle_ref,
    traces,
    late,
    chosen,
    terms,
    raw,
    part,
    arrived,
    merged,
    beside,
    joined,
    series,
    tail,
    load_sem,
    trace_sem,
    pair_send,
    pair_recv,
    beside_send,
    beside_recv,
    own_send,
    own_recv,
    sum_send,
    sum_recv,
):
    width = traces.shape[1]
    depth = math.gcd(channels, 256)
    each, lags = template_ref.shape
    pairs = devices // 2
    quads = devices // 4
    me = lax.axis_index("tm")
    core = lax.rem(me, 2)
    pair = me // 2
    quad = pair // 2
    side = lax.rem(pair, 2)
    partner = me + 1 - 2 * core
    blocks = width // LANES
    window = blocks + REACH // LANES
    outer = devices * blocks
    loads = [
        pltpu.make_async_copy(source, target, load_sem.at[i])
        for i, (source, target) in enumerate(
            (
                (moveouts_hbm, moveouts_ref),
                (mask_hbm, mask_ref),
                (template_hbm, template_ref),
                (first_hbm, first_ref),
                (forward_hbm, forward_ref),
                (twiddle_hbm, twiddle_ref),
                (back_hbm, back_ref),
                (last_hbm, last_ref),
            )
        )
    ]
    barrier = pltpu.get_barrier_semaphore()

    fetches = [
        pltpu.make_async_copy(
            traces_hbm.at[p * LANES : (p + 1) * LANES], traces.at[p * LANES : (p + 1) * LANES], trace_sem.at[p]
        )
        for p in range(channels // LANES)
    ]
    first_rows = depth // LANES
    for load in loads[:1] + fetches[:first_rows] + loads[1:2] + fetches[first_rows:] + loads[2:]:
        load.start()

    def greet(i, _):
        target = 2 * lax.rem(pair + i, pairs) + core
        pl.semaphore_signal(barrier, inc=1, device_id={"tm": target}, device_id_type=pl.DeviceIdType.MESH)
        return 0

    pl.semaphore_signal(barrier, inc=1, device_id={"tm": partner}, device_id_type=pl.DeviceIdType.MESH)
    lax.fori_loop(1, pairs, greet, 0)

    def to_partner(g):
        return pltpu.make_async_remote_copy(
            src_ref=part.at[1 - core, g],
            dst_ref=arrived.at[g],
            send_sem=pair_send.at[g],
            recv_sem=pair_recv.at[g],
            device_id={"tm": partner},
            device_id_type=pl.DeviceIdType.MESH,
        )

    common, alone = REACH // LANES * each, 2 * blocks * each
    common_at = pl.multiple_of((1 - side) * alone, each)
    alone_at = pl.multiple_of(side * common, each)

    def to_beside(q):
        return pltpu.make_async_remote_copy(
            src_ref=merged.at[2 * q + 1 - side, pl.ds(common_at, common)],
            dst_ref=beside.at[q],
            send_sem=beside_send.at[q],
            recv_sem=beside_recv.at[q],
            device_id={"tm": 2 * (2 * quad + 1 - side) + core},
            device_id_type=pl.DeviceIdType.MESH,
        )

    def alone_copy(g, source_quad, source_side):
        return pltpu.make_async_remote_copy(
            src_ref=merged.at[g, pl.ds(alone_at, alone)],
            dst_ref=joined.at[
                source_quad, pl.ds(pl.multiple_of(source_side * (alone + common), each), alone)
            ],
            send_sem=own_send.at[g],
            recv_sem=own_recv.at[2 * source_quad + source_side],
            device_id={"tm": 2 * g + core},
            device_id_type=pl.DeviceIdType.MESH,
        )

    def sum_copy(q, source_quad):
        return pltpu.make_async_remote_copy(
            src_ref=merged.at[2 * q + side, pl.ds(common_at, common)],
            dst_ref=joined.at[source_quad, alone : alone + common],
            send_sem=sum_send.at[q],
            recv_sem=sum_recv.at[source_quad],
            device_id={"tm": 2 * (2 * q + side) + core},
            device_id_type=pl.DeviceIdType.MESH,
        )

    def in_order(body):
        def visit(q, _):
            body(q)
            return 0

        lax.fori_loop(0, quad, visit, 0)
        lax.fori_loop(quad + 1, quads, visit, 0)

    loads[0].wait()
    for p in range(channels // LANES):
        row = (REACH - 1) - moveouts_ref[:, p * LANES : (p + 1) * LANES]
        late[p * LANES : (p + 1) * LANES, :] = jnp.broadcast_to(row, (LANES, LANES)).T
    count = mask_ref.shape[0]
    hops = REACH // LANES // COARSE

    def choose():
        loads[1].wait()
        coarse = ((REACH - 1) - moveouts_ref[...]) // (COARSE * LANES)
        for h in range(hops):
            chosen[h * count : (h + 1) * count, :] = (
                jnp.where(coarse == h, mask_ref[...], 0).astype(f32).astype(bf16)
            )

    fine = blocks + COARSE
    span = 2 if fine % 2 == 0 else 1

    def combine(c):
        one = chosen[:, c * depth : (c + 1) * depth]
        double = jnp.concatenate([one, one], axis=1)
        for b in range(0, fine, span):
            column = slice(b * LANES, (b + span) * LANES)
            value = jnp.dot(
                double, terms[2 * c * depth : 2 * (c + 1) * depth, column], preferred_element_type=f32
            )
            raw[:, column] = value if c == 0 else raw[:, column] + value

    for c in range(channels // depth):
        for p in range(c * depth // LANES, (c + 1) * depth // LANES):
            fetches[p].wait()
        if c == 1:
            choose()
        for row in range(0, depth, 8):
            shift(traces, late, terms, c * depth + row, 2 * c * depth + row, depth)
        if c > 0:
            combine(c - 1)
    if channels == depth:
        choose()
    combine(channels // depth - 1)

    def stacked(b):
        found = [h for h in range(hops) if 0 <= b - COARSE * h < fine]
        return sum(
            raw[h * count : (h + 1) * count, (b - COARSE * h) * LANES : (b - COARSE * h + 1) * LANES]
            for h in found
        )

    span = 2 if window % 2 == 0 else 1
    for b in range(0, window, span):
        added = [stacked(b + j) for j in range(span)]
        for owner in range(devices):
            part[owner % 2, owner // 2, b * each : (b + span) * each, :] = jnp.concatenate(
                [value[owner * each : (owner + 1) * each] for value in added], axis=0
            )
    pl.semaphore_wait(barrier, pairs)

    def first_send(q):
        to_partner(2 * q + 1 - side).start()
        to_partner(2 * q + side).start()

    in_order(first_send)
    first_send(quad)
    rows, more = window * each, blocks * each

    def merge(g):
        to_partner(g).wait_recv()
        own, other = part[core, g], arrived[g]
        early = jnp.where(core == 0, own, other)
        later = jnp.where(core == 0, other, own)
        merged[g, 0:more] = early[:more]
        merged[g, more:rows] = early[more:] + later[: rows - more]
        merged[g, rows : rows + more] = later[rows - more :]

    early = jnp.where(quad == quads // 2, quad, 0)

    def second_send(q):
        merge(2 * q + 1 - side)
        to_beside(q).start()
        merge(2 * q + side)

        @pl.when((q == 0) | (q > quad) | (q + 1 == early))
        def _():
            alone_copy(2 * q + side, quad, side).start()

        @pl.when(q == 0)
        def _():
            alone_copy(2 * q + 1 - side, quad, side).start()

    in_order(second_send)
    merge(2 * quad + 1 - side)
    to_beside(quad).start()
    alone_copy(2 * quad + 1 - side, quad, side).start()
    merge(pair)

    for load in loads[2:]:
        load.wait()
    cosine, sine = twiddle_ref[0], twiddle_ref[1]
    kept = cosine.shape[0]
    values = template_ref[...]
    count = lags // LANES
    for b in range(count):
        series[b * each : (b + 1) * each, :] = values[:, b * LANES : (b + 1) * LANES]
    series[count * each :, :] = jnp.zeros(((outer - count) * each, LANES), f32)
    energy = jnp.sqrt(jnp.sum(values * values, axis=1, keepdims=True) + 1e-06)
    factor = 1.0 / (outer * LANES * math.sqrt(channels) * energy)

    def columns():
        return [series[pl.ds(k, outer, stride=each), :] for k in range(each)]

    templ = transform(columns(), first_ref, forward_ref, cosine, sine)

    def add_beside(q):
        to_beside(q).wait_recv()
        here = (2 * q + side, pl.ds(common_at, common))
        merged[here] = merged[here] + beside[q]

    def third_send(q):
        add_beside(q)
        sum_copy(q, quad).start()

        @pl.when((q + 1 < quad) & (q + 2 != early))
        def _():
            alone_copy(2 * (q + 1) + side, quad, side).start()

        @pl.when(q + 1 < quad)
        def _():
            alone_copy(2 * (q + 1) + 1 - side, quad, side).start()

    def fourth_send(q, _):
        alone_copy(2 * q + 1 - side, quad, side).start()
        return 0

    lax.fori_loop(quad + 1, quads, fourth_send, 0)
    in_order(third_send)

    add_beside(quad)
    joined[quad, alone : alone + common] = merged[pair, pl.ds(common_at, common)]
    joined[quad, pl.ds(pl.multiple_of(side * (alone + common), each), alone)] = merged[
        pair, pl.ds(alone_at, alone)
    ]

    def finish(q):
        alone_copy(2 * q + 1 - side, q, 1 - side).wait()
        alone_copy(2 * q + side, q, side).wait()
        to_beside(q).wait_send()
        sum_copy(q, q).wait()

    in_order(finish)
    alone_copy(2 * quad + 1 - side, quad, 1 - side).wait()
    to_beside(quad).wait_send()

    def leave(g, _):
        to_partner(g).wait_send()
        return 0

    lax.fori_loop(0, pairs, leave, 0)
    series[...] = jnp.zeros(series.shape, f32)
    local = 2 * blocks
    wide = 2 * local + REACH // LANES
    for source in range(quads):
        for b in range(0, wide, local):
            taken = min(local, wide - b)
            block = (2 * source * local + b - REACH // LANES) % outer
            here = slice(block * each, (block + taken) * each)
            series[here, :] = series[here, :] + joined[source, b * each : (b + taken) * each, :]
    stack = transform(columns(), first_ref, forward_ref, cosine, sine)
    stack_re, stack_im = stack[:, :LANES], stack[:, LANES:]
    templ_re, templ_im = templ[:, :LANES], templ[:, LANES:]
    product = jnp.concatenate(
        [stack_re * templ_re + stack_im * templ_im, stack_im * templ_re - stack_re * templ_im], axis=1
    )
    high, low = split(product)
    back = jnp.dot(jnp.concatenate([high, low, high], axis=1), back_ref[...], preferred_element_type=f32)
    turned = []
    for k in range(each):
        re = back[k * kept : (k + 1) * kept, :LANES]
        im = back[k * kept : (k + 1) * kept, LANES:]
        turned.append(jnp.concatenate([re * cosine - im * sine, re * sine + im * cosine], axis=0))
    high, low = split(jnp.concatenate(turned, axis=1))
    final = jnp.dot(last_ref[...], jnp.concatenate([high, high, low], axis=0), preferred_element_type=f32)
    for k in range(each):
        tail[pl.ds(k, count, stride=each), :] = final[:, k * LANES : (k + 1) * LANES]
    for b in range(count):
        out_ref[:, b * LANES : (b + 1) * LANES] = tail[b * each : (b + 1) * each, :] * factor


def tables(length, lags):
    outer = length // LANES
    turn = 2.0 * math.pi
    kept = (outer // 2 + 1 + 7) // 8 * 8
    weight = np.where(np.arange(kept) % (outer // 2) == 0, 1.0, 2.0) * (np.arange(kept) <= outer // 2)
    ramp = np.arange(kept)[:, None] * np.arange(outer)[None, :] % outer * (turn / outer)
    wide = np.arange(LANES)[:, None] * np.arange(LANES)[None, :] % LANES * (turn / LANES)
    twist = np.arange(kept)[:, None] * np.arange(LANES)[None, :] % length * (turn / length)
    first = split_table(np.concatenate([np.cos(ramp), -np.sin(ramp)], axis=0))
    cosine, sine = np.cos(wide), np.sin(wide)
    forward = split_table(np.block([[cosine, -sine], [sine, cosine]]))
    back = split_table(np.block([[cosine, sine], [-sine, cosine]]))
    shown = ramp[:, : lags // LANES].T
    last = split_table(np.concatenate([np.cos(shown) * weight, -np.sin(shown) * weight], axis=1))
    return (
        np.concatenate([first[0], first[1], first[0]], axis=1),
        np.concatenate([forward[0], forward[0], forward[1]], axis=0),
        np.concatenate([back[0], back[0], back[1]], axis=0),
        np.concatenate([last[0], last[1], last[0]], axis=1),
        np.stack([np.cos(twist), np.sin(twist)]).astype(np.float32),
    )


def on_device(devices, traces, templates, moveouts, masks):
    channels, width = traces.shape
    each, lags = templates.shape
    blocks = width // LANES
    outer = devices * blocks
    window = blocks + REACH // LANES
    pairs, quads = devices // 2, devices // 4
    loaded = [moveouts[None, :], masks, templates, *[jnp.asarray(table) for table in tables(outer * LANES, lags)]]
    alone, common = 2 * blocks * each, REACH // LANES * each
    return pl.pallas_call(
        functools.partial(kernel, devices, channels),
        in_specs=[pl.BlockSpec(memory_space=pl.ANY) for _ in range(len(loaded) + 1)],
        out_specs=pl.BlockSpec(memory_space=pltpu.VMEM),
        out_shape=pltpu.VMEM((each, lags), f32),
        scratch_shapes=[
            *[pltpu.VMEM(value.shape, value.dtype) for value in loaded],
            pltpu.VMEM((channels, width), f32),
            pltpu.VMEM((channels, LANES), jnp.int32),
            pltpu.VMEM((REACH // LANES // COARSE * masks.shape[0], channels), bf16),
            pltpu.VMEM((2 * channels, (blocks + COARSE) * LANES), bf16),
            pltpu.VMEM((REACH // LANES // COARSE * masks.shape[0], (blocks + COARSE) * LANES), f32),
            pltpu.VMEM((2, pairs, window * each, LANES), f32),
            pltpu.VMEM((pairs, window * each, LANES), f32),
            pltpu.VMEM((pairs, alone + common, LANES), f32),
            pltpu.VMEM((quads, common, LANES), f32),
            pltpu.VMEM((quads, 2 * alone + common, LANES), f32),
            pltpu.VMEM((outer * each, LANES), f32),
            pltpu.VMEM((lags // LANES * each, LANES), f32),
            pltpu.SemaphoreType.DMA((len(loaded),)),
            pltpu.SemaphoreType.DMA((channels // LANES,)),
            *[pltpu.SemaphoreType.DMA((count,)) for count in (pairs, pairs, quads, quads, pairs, pairs, quads, quads)],
        ],
        compiler_params=pltpu.CompilerParams(collective_id=0, has_side_effects=True),
        name="detect",
    )(*loaded[:2], traces, *loaded[2:])


def solution(mesh):
    return jax.shard_map(
        functools.partial(on_device, mesh.shape["tm"]),
        mesh=mesh,
        in_specs=(P("grp", "tm"), P("tm", None), P("grp"), P(None, "grp")),
        out_specs=P("tm", "grp"),
        check_vma=False,
    )
```

```python
import functools
import math

import jax
import jax.numpy as jnp
import numpy as np
from jax import lax
from jax.experimental import pallas as pl
from jax.experimental.pallas import tpu as pltpu
from jax.sharding import PartitionSpec as P

f32, bf16 = jnp.float32, jnp.bfloat16
LANES = 128
REACH = 2048
COARSE = 4


def split(value):
    high = value.astype(bf16)
    return high, (value - high.astype(f32)).astype(bf16)


def split_table(table):
    high = table.astype(jnp.bfloat16)
    return high, (table - high.astype(np.float64)).astype(jnp.bfloat16)


def transform(rows, first_ref, forward_ref, cosine, sine):
    outer = cosine.shape[0]
    high, low = split(jnp.concatenate(rows, axis=1))
    first = jnp.dot(first_ref[...], jnp.concatenate([high, high, low], axis=0), preferred_element_type=f32)
    turned = []
    for r in range(len(rows)):
        re = first[:outer, r * LANES : (r + 1) * LANES]
        im = first[outer:, r * LANES : (r + 1) * LANES]
        turned.append(jnp.concatenate([re * cosine + im * sine, im * cosine - re * sine], axis=1))
    high, low = split(jnp.concatenate(turned, axis=0))
    return jnp.dot(jnp.concatenate([high, low, high], axis=1), forward_ref[...], preferred_element_type=f32)


def shift(traces, late, terms, row, target, depth):
    rows = 8
    blocks = traces.shape[1] // LANES
    here = slice(row, row + rows)
    delay = late[here, :]
    lane = lax.broadcasted_iota(jnp.int32, (rows, LANES), 1)
    inner = (delay & (LANES - 1)) + 1
    index = (lane - inner) & (LANES - 1)
    keep = lane >= inner
    turned = [
        jnp.take_along_axis(traces[here, b * LANES : (b + 1) * LANES], index, axis=1, mode="promise_in_bounds")
        for b in range(blocks)
    ]
    zero = jnp.zeros((rows, LANES), f32)
    moved = [
        jnp.where(keep, turned[b] if b < blocks else zero, turned[b - 1] if b > 0 else zero)
        for b in range(blocks + 1)
    ]
    hop = 1
    while hop < COARSE:
        chosen = ((delay // LANES) & hop) != 0
        moved = [
            jnp.where(
                chosen,
                moved[b - hop] if b >= hop else zero,
                moved[b] if b < len(moved) else zero,
            )
            for b in range(len(moved) + hop)
        ]
        hop *= 2
    span = 2 if len(moved) % 2 == 0 else 1
    for b in range(0, len(moved), span):
        high, low = split(jnp.concatenate(moved[b : b + span], axis=1))
        column = slice(b * LANES, (b + span) * LANES)
        terms[target : target + rows, column] = high
        terms[target + depth : target + depth + rows, column] = low


def kernel(
    devices,
    channels,
    moveouts_hbm,
    mask_hbm,
    traces_hbm,
    template_hbm,
    first_hbm,
    forward_hbm,
    back_hbm,
    last_hbm,
    twiddle_hbm,
    out_ref,
    moveouts_ref,
    mask_ref,
    template_ref,
    first_ref,
    forward_ref,
    back_ref,
    last_ref,
    twiddle_ref,
    traces,
    late,
    chosen,
    terms,
    raw,
    part,
    arrived,
    merged,
    beside,
    joined,
    series,
    tail,
    load_sem,
    trace_sem,
    pair_send,
    pair_recv,
    beside_send,
    beside_recv,
    own_send,
    own_recv,
    sum_send,
    sum_recv,
):
    width = traces.shape[1]
    depth = math.gcd(channels, 256)
    each, lags = template_ref.shape
    pairs = devices // 2
    quads = devices // 4
    me = lax.axis_index("tm")
    core = lax.rem(me, 2)
    pair = me // 2
    quad = pair // 2
    side = lax.rem(pair, 2)
    partner = me + 1 - 2 * core
    blocks = width // LANES
    window = blocks + REACH // LANES
    outer = devices * blocks
    loads = [
        pltpu.make_async_copy(source, target, load_sem.at[i])
        for i, (source, target) in enumerate(
            (
                (moveouts_hbm, moveouts_ref),
                (mask_hbm, mask_ref),
                (template_hbm, template_ref),
                (first_hbm, first_ref),
                (forward_hbm, forward_ref),
                (twiddle_hbm, twiddle_ref),
                (back_hbm, back_ref),
                (last_hbm, last_ref),
            )
        )
    ]
    barrier = pltpu.get_barrier_semaphore()

    fetches = [
        pltpu.make_async_copy(
            traces_hbm.at[p * LANES : (p + 1) * LANES], traces.at[p * LANES : (p + 1) * LANES], trace_sem.at[p]
        )
        for p in range(channels // LANES)
    ]
    first_rows = depth // LANES
    for load in loads[:1] + fetches[:first_rows] + loads[1:2] + fetches[first_rows:] + loads[2:]:
        load.start()

    def greet(i, _):
        target = 2 * lax.rem(pair + i, pairs) + core
        pl.semaphore_signal(barrier, inc=1, device_id={"tm": target}, device_id_type=pl.DeviceIdType.MESH)
        return 0

    pl.semaphore_signal(barrier, inc=1, device_id={"tm": partner}, device_id_type=pl.DeviceIdType.MESH)
    lax.fori_loop(1, pairs, greet, 0)

    def to_partner(g):
        return pltpu.make_async_remote_copy(
            src_ref=part.at[1 - core, g],
            dst_ref=arrived.at[g],
            send_sem=pair_send.at[g],
            recv_sem=pair_recv.at[g],
            device_id={"tm": partner},
            device_id_type=pl.DeviceIdType.MESH,
        )

    common, alone = REACH // LANES * each, 2 * blocks * each
    common_at = pl.multiple_of((1 - side) * alone, each)
    alone_at = pl.multiple_of(side * common, each)

    def to_beside(q):
        return pltpu.make_async_remote_copy(
            src_ref=merged.at[2 * q + 1 - side, pl.ds(common_at, common)],
            dst_ref=beside.at[q],
            send_sem=beside_send.at[q],
            recv_sem=beside_recv.at[q],
            device_id={"tm": 2 * (2 * quad + 1 - side) + core},
            device_id_type=pl.DeviceIdType.MESH,
        )

    def alone_copy(g, source_quad, source_side):
        return pltpu.make_async_remote_copy(
            src_ref=merged.at[g, pl.ds(alone_at, alone)],
            dst_ref=joined.at[
                source_quad, pl.ds(pl.multiple_of(source_side * (alone + common), each), alone)
            ],
            send_sem=own_send.at[g],
            recv_sem=own_recv.at[2 * source_quad + source_side],
            device_id={"tm": 2 * g + core},
            device_id_type=pl.DeviceIdType.MESH,
        )

    def sum_copy(q, source_quad):
        return pltpu.make_async_remote_copy(
            src_ref=merged.at[2 * q + side, pl.ds(common_at, common)],
            dst_ref=joined.at[source_quad, alone : alone + common],
            send_sem=sum_send.at[q],
            recv_sem=sum_recv.at[source_quad],
            device_id={"tm": 2 * (2 * q + side) + core},
            device_id_type=pl.DeviceIdType.MESH,
        )

    def in_order(body):
        def visit(q, _):
            body(q)
            return 0

        lax.fori_loop(0, quad, visit, 0)
        lax.fori_loop(quad + 1, quads, visit, 0)

    loads[0].wait()
    for p in range(channels // LANES):
        row = (REACH - 1) - moveouts_ref[:, p * LANES : (p + 1) * LANES]
        late[p * LANES : (p + 1) * LANES, :] = jnp.broadcast_to(row, (LANES, LANES)).T
    count = mask_ref.shape[0]
    hops = REACH // LANES // COARSE

    def choose():
        loads[1].wait()
        coarse = ((REACH - 1) - moveouts_ref[...]) // (COARSE * LANES)
        for h in range(hops):
            chosen[h * count : (h + 1) * count, :] = (
                jnp.where(coarse == h, mask_ref[...], 0).astype(f32).astype(bf16)
            )

    fine = blocks + COARSE
    span = 2 if fine % 2 == 0 else 1

    def combine(c):
        one = chosen[:, c * depth : (c + 1) * depth]
        double = jnp.concatenate([one, one], axis=1)
        for b in range(0, fine, span):
            column = slice(b * LANES, (b + span) * LANES)
            value = jnp.dot(
                double, terms[2 * c * depth : 2 * (c + 1) * depth, column], preferred_element_type=f32
            )
            raw[:, column] = value if c == 0 else raw[:, column] + value

    for c in range(channels // depth):
        for p in range(c * depth // LANES, (c + 1) * depth // LANES):
            fetches[p].wait()
        if c == 1:
            choose()
        for row in range(0, depth, 8):
            shift(traces, late, terms, c * depth + row, 2 * c * depth + row, depth)
        if c > 0:
            combine(c - 1)
    if channels == depth:
        choose()
    combine(channels // depth - 1)

    def stacked(b):
        found = [h for h in range(hops) if 0 <= b - COARSE * h < fine]
        return sum(
            raw[h * count : (h + 1) * count, (b - COARSE * h) * LANES : (b - COARSE * h + 1) * LANES]
            for h in found
        )

    span = 2 if window % 2 == 0 else 1
    for b in range(0, window, span):
        added = [stacked(b + j) for j in range(span)]
        for owner in range(devices):
            part[owner % 2, owner // 2, b * each : (b + span) * each, :] = jnp.concatenate(
                [value[owner * each : (owner + 1) * each] for value in added], axis=0
            )
    pl.semaphore_wait(barrier, pairs)

    def first_send(q):
        to_partner(2 * q + 1 - side).start()
        to_partner(2 * q + side).start()

    in_order(first_send)
    first_send(quad)
    rows, more = window * each, blocks * each

    def merge(g):
        to_partner(g).wait_recv()
        own, other = part[core, g], arrived[g]
        early = jnp.where(core == 0, own, other)
        later = jnp.where(core == 0, other, own)
        merged[g, 0:more] = early[:more]
        merged[g, more:rows] = early[more:] + later[: rows - more]
        merged[g, rows : rows + more] = later[rows - more :]

    half = quads // 2

    def at_once(q):
        return (q < quad) & ((q == 0) | ((q < half) & (quad > half)))

    def second_send(q):
        merge(2 * q + 1 - side)
        to_beside(q).start()
        merge(2 * q + side)

        @pl.when(q > quad)
        def _():
            alone_copy(2 * q + side, quad, side).start()

        @pl.when(at_once(q))
        def _():
            alone_copy(2 * q, quad, side).start()
            alone_copy(2 * q + 1, quad, side).start()

    in_order(second_send)
    merge(2 * quad + 1 - side)
    to_beside(quad).start()
    alone_copy(2 * quad + 1 - side, quad, side).start()
    merge(pair)

    for load in loads[2:]:
        load.wait()
    cosine, sine = twiddle_ref[0], twiddle_ref[1]
    kept = cosine.shape[0]
    values = template_ref[...]
    count = lags // LANES
    for b in range(count):
        series[b * each : (b + 1) * each, :] = values[:, b * LANES : (b + 1) * LANES]
    series[count * each :, :] = jnp.zeros(((outer - count) * each, LANES), f32)
    energy = jnp.sqrt(jnp.sum(values * values, axis=1, keepdims=True) + 1e-06)
    factor = 1.0 / (outer * LANES * math.sqrt(channels) * energy)

    def columns():
        return [series[pl.ds(k, outer, stride=each), :] for k in range(each)]

    templ = transform(columns(), first_ref, forward_ref, cosine, sine)

    def add_beside(q):
        to_beside(q).wait_recv()
        here = (2 * q + side, pl.ds(common_at, common))
        merged[here] = merged[here] + beside[q]

    def third_send(q):
        add_beside(q)
        sum_copy(q, quad).start()

        @pl.when((q + 1 < quad) & jnp.logical_not(at_once(q + 1)))
        def _():
            alone_copy(2 * (q + 1) + side, quad, side).start()
            alone_copy(2 * (q + 1) + 1 - side, quad, side).start()

    def fourth_send(q, _):
        alone_copy(2 * q + 1 - side, quad, side).start()
        return 0

    lax.fori_loop(quad + 1, quads, fourth_send, 0)
    in_order(third_send)

    add_beside(quad)
    joined[quad, alone : alone + common] = merged[pair, pl.ds(common_at, common)]
    joined[quad, pl.ds(pl.multiple_of(side * (alone + common), each), alone)] = merged[
        pair, pl.ds(alone_at, alone)
    ]

    def leave(g, _):
        to_partner(g).wait_send()
        return 0

    lax.fori_loop(0, pairs, leave, 0)
    series[...] = jnp.zeros(series.shape, f32)

    def finish(q):
        alone_copy(2 * q + 1 - side, q, 1 - side).wait()
        alone_copy(2 * q + side, q, side).wait()
        to_beside(q).wait_send()
        sum_copy(q, q).wait()

    in_order(finish)
    alone_copy(2 * quad + 1 - side, quad, 1 - side).wait()
    to_beside(quad).wait_send()

    local = 2 * blocks
    wide = 2 * local + REACH // LANES
    for source in range(quads):
        for b in range(0, wide, local):
            taken = min(local, wide - b)
            block = (2 * source * local + b - REACH // LANES) % outer
            here = slice(block * each, (block + taken) * each)
            series[here, :] = series[here, :] + joined[source, b * each : (b + taken) * each, :]
    stack = transform(columns(), first_ref, forward_ref, cosine, sine)
    stack_re, stack_im = stack[:, :LANES], stack[:, LANES:]
    templ_re, templ_im = templ[:, :LANES], templ[:, LANES:]
    product = jnp.concatenate(
        [stack_re * templ_re + stack_im * templ_im, stack_im * templ_re - stack_re * templ_im], axis=1
    )
    high, low = split(product)
    back = jnp.dot(jnp.concatenate([high, low, high], axis=1), back_ref[...], preferred_element_type=f32)
    turned = []
    for k in range(each):
        re = back[k * kept : (k + 1) * kept, :LANES]
        im = back[k * kept : (k + 1) * kept, LANES:]
        turned.append(jnp.concatenate([re * cosine - im * sine, re * sine + im * cosine], axis=0))
    high, low = split(jnp.concatenate(turned, axis=1))
    final = jnp.dot(last_ref[...], jnp.concatenate([high, high, low], axis=0), preferred_element_type=f32)
    for k in range(each):
        tail[pl.ds(k, count, stride=each), :] = final[:, k * LANES : (k + 1) * LANES]
    for b in range(count):
        out_ref[:, b * LANES : (b + 1) * LANES] = tail[b * each : (b + 1) * each, :] * factor


def tables(length, lags):
    outer = length // LANES
    turn = 2.0 * math.pi
    kept = (outer // 2 + 1 + 7) // 8 * 8
    weight = np.where(np.arange(kept) % (outer // 2) == 0, 1.0, 2.0) * (np.arange(kept) <= outer // 2)
    ramp = np.arange(kept)[:, None] * np.arange(outer)[None, :] % outer * (turn / outer)
    wide = np.arange(LANES)[:, None] * np.arange(LANES)[None, :] % LANES * (turn / LANES)
    twist = np.arange(kept)[:, None] * np.arange(LANES)[None, :] % length * (turn / length)
    first = split_table(np.concatenate([np.cos(ramp), -np.sin(ramp)], axis=0))
    cosine, sine = np.cos(wide), np.sin(wide)
    forward = split_table(np.block([[cosine, -sine], [sine, cosine]]))
    back = split_table(np.block([[cosine, sine], [-sine, cosine]]))
    shown = ramp[:, : lags // LANES].T
    last = split_table(np.concatenate([np.cos(shown) * weight, -np.sin(shown) * weight], axis=1))
    return (
        np.concatenate([first[0], first[1], first[0]], axis=1),
        np.concatenate([forward[0], forward[0], forward[1]], axis=0),
        np.concatenate([back[0], back[0], back[1]], axis=0),
        np.concatenate([last[0], last[1], last[0]], axis=1),
        np.stack([np.cos(twist), np.sin(twist)]).astype(np.float32),
    )


def on_device(devices, traces, templates, moveouts, masks):
    channels, width = traces.shape
    each, lags = templates.shape
    blocks = width // LANES
    outer = devices * blocks
    window = blocks + REACH // LANES
    pairs, quads = devices // 2, devices // 4
    loaded = [moveouts[None, :], masks, templates, *[jnp.asarray(table) for table in tables(outer * LANES, lags)]]
    alone, common = 2 * blocks * each, REACH // LANES * each
    return pl.pallas_call(
        functools.partial(kernel, devices, channels),
        in_specs=[pl.BlockSpec(memory_space=pl.ANY) for _ in range(len(loaded) + 1)],
        out_specs=pl.BlockSpec(memory_space=pltpu.VMEM),
        out_shape=pltpu.VMEM((each, lags), f32),
        scratch_shapes=[
            *[pltpu.VMEM(value.shape, value.dtype) for value in loaded],
            pltpu.VMEM((channels, width), f32),
            pltpu.VMEM((channels, LANES), jnp.int32),
            pltpu.VMEM((REACH // LANES // COARSE * masks.shape[0], channels), bf16),
            pltpu.VMEM((2 * channels, (blocks + COARSE) * LANES), bf16),
            pltpu.VMEM((REACH // LANES // COARSE * masks.shape[0], (blocks + COARSE) * LANES), f32),
            pltpu.VMEM((2, pairs, window * each, LANES), f32),
            pltpu.VMEM((pairs, window * each, LANES), f32),
            pltpu.VMEM((pairs, alone + common, LANES), f32),
            pltpu.VMEM((quads, common, LANES), f32),
            pltpu.VMEM((quads, 2 * alone + common, LANES), f32),
            pltpu.VMEM((outer * each, LANES), f32),
            pltpu.VMEM((lags // LANES * each, LANES), f32),
            pltpu.SemaphoreType.DMA((len(loaded),)),
            pltpu.SemaphoreType.DMA((channels // LANES,)),
            *[pltpu.SemaphoreType.DMA((count,)) for count in (pairs, pairs, quads, quads, pairs, pairs, quads, quads)],
        ],
        compiler_params=pltpu.CompilerParams(collective_id=0, has_side_effects=True),
        name="detect",
    )(*loaded[:2], traces, *loaded[2:])


def solution(mesh):
    return jax.shard_map(
        functools.partial(on_device, mesh.shape["tm"]),
        mesh=mesh,
        in_specs=(P("grp", "tm"), P("tm", None), P("grp"), P(None, "grp")),
        out_specs=P("tm", "grp"),
        check_vma=False,
    )
```

```python
import functools
import math

import jax
import jax.numpy as jnp
import numpy as np
from jax import lax
from jax.experimental import pallas as pl
from jax.experimental.pallas import tpu as pltpu
from jax.sharding import PartitionSpec as P

f32, bf16 = jnp.float32, jnp.bfloat16
LANES = 128
REACH = 2048
COARSE = 4


def split(value):
    high = value.astype(bf16)
    return high, (value - high.astype(f32)).astype(bf16)


def split_table(table):
    high = table.astype(jnp.bfloat16)
    return high, (table - high.astype(np.float64)).astype(jnp.bfloat16)


def transform(rows, first_ref, forward_ref, cosine, sine):
    outer = cosine.shape[0]
    high, low = split(jnp.concatenate(rows, axis=1))
    first = jnp.dot(first_ref[...], jnp.concatenate([high, high, low], axis=0), preferred_element_type=f32)
    turned = []
    for r in range(len(rows)):
        re = first[:outer, r * LANES : (r + 1) * LANES]
        im = first[outer:, r * LANES : (r + 1) * LANES]
        turned.append(jnp.concatenate([re * cosine + im * sine, im * cosine - re * sine], axis=1))
    high, low = split(jnp.concatenate(turned, axis=0))
    return jnp.dot(jnp.concatenate([high, low, high], axis=1), forward_ref[...], preferred_element_type=f32)


def shift(traces, late, terms, row, target, depth):
    rows = 8
    blocks = traces.shape[1] // LANES
    here = slice(row, row + rows)
    delay = late[here, :]
    lane = lax.broadcasted_iota(jnp.int32, (rows, LANES), 1)
    inner = (delay & (LANES - 1)) + 1
    index = (lane - inner) & (LANES - 1)
    keep = lane >= inner
    turned = [
        jnp.take_along_axis(traces[here, b * LANES : (b + 1) * LANES], index, axis=1, mode="promise_in_bounds")
        for b in range(blocks)
    ]
    zero = jnp.zeros((rows, LANES), f32)
    moved = [
        jnp.where(keep, turned[b] if b < blocks else zero, turned[b - 1] if b > 0 else zero)
        for b in range(blocks + 1)
    ]
    hop = 1
    while hop < COARSE:
        chosen = ((delay // LANES) & hop) != 0
        moved = [
            jnp.where(
                chosen,
                moved[b - hop] if b >= hop else zero,
                moved[b] if b < len(moved) else zero,
            )
            for b in range(len(moved) + hop)
        ]
        hop *= 2
    span = 2 if len(moved) % 2 == 0 else 1
    for b in range(0, len(moved), span):
        high, low = split(jnp.concatenate(moved[b : b + span], axis=1))
        column = slice(b * LANES, (b + span) * LANES)
        terms[target : target + rows, column] = high
        terms[target + depth : target + depth + rows, column] = low


def kernel(
    devices,
    channels,
    moveouts_hbm,
    mask_hbm,
    traces_hbm,
    template_hbm,
    first_hbm,
    forward_hbm,
    back_hbm,
    last_hbm,
    twiddle_hbm,
    out_ref,
    moveouts_ref,
    mask_ref,
    template_ref,
    first_ref,
    forward_ref,
    back_ref,
    last_ref,
    twiddle_ref,
    traces,
    late,
    chosen,
    terms,
    raw,
    part,
    arrived,
    merged,
    beside,
    joined,
    series,
    tail,
    load_sem,
    trace_sem,
    pair_send,
    pair_recv,
    beside_send,
    beside_recv,
    own_send,
    own_recv,
    sum_send,
    sum_recv,
):
    width = traces.shape[1]
    depth = math.gcd(channels, 256)
    each, lags = template_ref.shape
    pairs = devices // 2
    quads = devices // 4
    me = lax.axis_index("tm")
    core = lax.rem(me, 2)
    pair = me // 2
    quad = pair // 2
    side = lax.rem(pair, 2)
    partner = me + 1 - 2 * core
    blocks = width // LANES
    window = blocks + REACH // LANES
    outer = devices * blocks
    loads = [
        pltpu.make_async_copy(source, target, load_sem.at[i])
        for i, (source, target) in enumerate(
            (
                (moveouts_hbm, moveouts_ref),
                (mask_hbm, mask_ref),
                (template_hbm, template_ref),
                (first_hbm, first_ref),
                (forward_hbm, forward_ref),
                (twiddle_hbm, twiddle_ref),
                (back_hbm, back_ref),
                (last_hbm, last_ref),
            )
        )
    ]
    barrier = pltpu.get_barrier_semaphore()

    fetches = [
        pltpu.make_async_copy(
            traces_hbm.at[p * LANES : (p + 1) * LANES], traces.at[p * LANES : (p + 1) * LANES], trace_sem.at[p]
        )
        for p in range(channels // LANES)
    ]
    first_rows = depth // LANES
    for load in loads[:1] + fetches[:first_rows] + loads[1:2] + fetches[first_rows:] + loads[2:]:
        load.start()

    def greet(i, _):
        target = 2 * lax.rem(pair + i, pairs) + core
        pl.semaphore_signal(barrier, inc=1, device_id={"tm": target}, device_id_type=pl.DeviceIdType.MESH)
        return 0

    pl.semaphore_signal(barrier, inc=1, device_id={"tm": partner}, device_id_type=pl.DeviceIdType.MESH)
    lax.fori_loop(1, pairs, greet, 0)

    def to_partner(g):
        return pltpu.make_async_remote_copy(
            src_ref=part.at[1 - core, g],
            dst_ref=arrived.at[g],
            send_sem=pair_send.at[g],
            recv_sem=pair_recv.at[g],
            device_id={"tm": partner},
            device_id_type=pl.DeviceIdType.MESH,
        )

    common, alone = REACH // LANES * each, 2 * blocks * each
    common_at = pl.multiple_of((1 - side) * alone, each)
    alone_at = pl.multiple_of(side * common, each)

    def to_beside(q):
        return pltpu.make_async_remote_copy(
            src_ref=merged.at[2 * q + 1 - side, pl.ds(common_at, common)],
            dst_ref=beside.at[q],
            send_sem=beside_send.at[q],
            recv_sem=beside_recv.at[q],
            device_id={"tm": 2 * (2 * quad + 1 - side) + core},
            device_id_type=pl.DeviceIdType.MESH,
        )

    def alone_copy(g, source_quad, source_side):
        return pltpu.make_async_remote_copy(
            src_ref=merged.at[g, pl.ds(alone_at, alone)],
            dst_ref=joined.at[
                source_quad, pl.ds(pl.multiple_of(source_side * (alone + common), each), alone)
            ],
            send_sem=own_send.at[g],
            recv_sem=own_recv.at[2 * source_quad + source_side],
            device_id={"tm": 2 * g + core},
            device_id_type=pl.DeviceIdType.MESH,
        )

    def sum_copy(q, source_quad):
        return pltpu.make_async_remote_copy(
            src_ref=merged.at[2 * q + side, pl.ds(common_at, common)],
            dst_ref=joined.at[source_quad, alone : alone + common],
            send_sem=sum_send.at[q],
            recv_sem=sum_recv.at[source_quad],
            device_id={"tm": 2 * (2 * q + side) + core},
            device_id_type=pl.DeviceIdType.MESH,
        )

    def in_order(body):
        def visit(q, _):
            body(q)
            return 0

        lax.fori_loop(0, quad, visit, 0)
        lax.fori_loop(quad + 1, quads, visit, 0)

    loads[0].wait()
    for p in range(channels // LANES):
        row = (REACH - 1) - moveouts_ref[:, p * LANES : (p + 1) * LANES]
        late[p * LANES : (p + 1) * LANES, :] = jnp.broadcast_to(row, (LANES, LANES)).T
    count = mask_ref.shape[0]
    hops = REACH // LANES // COARSE

    def choose():
        loads[1].wait()
        coarse = ((REACH - 1) - moveouts_ref[...]) // (COARSE * LANES)
        for h in range(hops):
            chosen[h * count : (h + 1) * count, :] = (
                jnp.where(coarse == h, mask_ref[...], 0).astype(f32).astype(bf16)
            )

    fine = blocks + COARSE
    span = 2 if fine % 2 == 0 else 1

    def combine(c):
        one = chosen[:, c * depth : (c + 1) * depth]
        double = jnp.concatenate([one, one], axis=1)
        for b in range(0, fine, span):
            column = slice(b * LANES, (b + span) * LANES)
            value = jnp.dot(
                double, terms[2 * c * depth : 2 * (c + 1) * depth, column], preferred_element_type=f32
            )
            raw[:, column] = value if c == 0 else raw[:, column] + value

    for c in range(channels // depth):
        for p in range(c * depth // LANES, (c + 1) * depth // LANES):
            fetches[p].wait()
        if c == 1:
            choose()
        for row in range(0, depth, 8):
            shift(traces, late, terms, c * depth + row, 2 * c * depth + row, depth)
        if c > 0:
            combine(c - 1)
    if channels == depth:
        choose()
    combine(channels // depth - 1)

    def stacked(b):
        found = [h for h in range(hops) if 0 <= b - COARSE * h < fine]
        return sum(
            raw[h * count : (h + 1) * count, (b - COARSE * h) * LANES : (b - COARSE * h + 1) * LANES]
            for h in found
        )

    span = 2 if window % 2 == 0 else 1
    for b in range(0, window, span):
        added = [stacked(b + j) for j in range(span)]
        for owner in range(devices):
            part[owner % 2, owner // 2, b * each : (b + span) * each, :] = jnp.concatenate(
                [value[owner * each : (owner + 1) * each] for value in added], axis=0
            )
    pl.semaphore_wait(barrier, pairs)

    def first_send(q):
        to_partner(2 * q + 1 - side).start()
        to_partner(2 * q + side).start()

    in_order(first_send)
    first_send(quad)
    rows, more = window * each, blocks * each

    def merge(g):
        to_partner(g).wait_recv()
        own, other = part[core, g], arrived[g]
        early = jnp.where(core == 0, own, other)
        later = jnp.where(core == 0, other, own)
        merged[g, 0:more] = early[:more]
        merged[g, more:rows] = early[more:] + later[: rows - more]
        merged[g, rows : rows + more] = later[rows - more :]

    half = quads // 2

    def at_once(q):
        return (q < quad) & ((q == 0) | ((q < half) & (quad > half)))

    def second_send(q):
        merge(2 * q + 1 - side)
        to_beside(q).start()
        merge(2 * q + side)

        @pl.when(q > quad)
        def _():
            alone_copy(2 * q + side, quad, side).start()

        @pl.when(at_once(q))
        def _():
            alone_copy(2 * q, quad, side).start()
            alone_copy(2 * q + 1, quad, side).start()

    in_order(second_send)
    merge(2 * quad + 1 - side)
    to_beside(quad).start()
    alone_copy(2 * quad + 1 - side, quad, side).start()
    merge(pair)

    for load in loads[2:]:
        load.wait()
    cosine, sine = twiddle_ref[0], twiddle_ref[1]
    kept = cosine.shape[0]
    values = template_ref[...]
    count = lags // LANES
    for b in range(count):
        series[b * each : (b + 1) * each, :] = values[:, b * LANES : (b + 1) * LANES]
    series[count * each :, :] = jnp.zeros(((outer - count) * each, LANES), f32)
    energy = jnp.sqrt(jnp.sum(values * values, axis=1, keepdims=True) + 1e-06)
    factor = 1.0 / (outer * LANES * math.sqrt(channels) * energy)

    def columns():
        return [series[pl.ds(k, outer, stride=each), :] for k in range(each)]

    templ = transform(columns(), first_ref, forward_ref, cosine, sine)

    def add_beside(q):
        to_beside(q).wait_recv()
        here = (2 * q + side, pl.ds(common_at, common))
        merged[here] = merged[here] + beside[q]

    def third_send(q):
        add_beside(q)
        sum_copy(q, quad).start()

        @pl.when((q + 1 < quad) & jnp.logical_not(at_once(q + 1)))
        def _():
            alone_copy(2 * (q + 1) + 1 - side, quad, side).start()
            alone_copy(2 * (q + 1) + side, quad, side).start()

    def fourth_send(q, _):
        alone_copy(2 * q + 1 - side, quad, side).start()
        return 0

    lax.fori_loop(quad + 1, quads, fourth_send, 0)
    in_order(third_send)

    add_beside(quad)
    joined[quad, alone : alone + common] = merged[pair, pl.ds(common_at, common)]
    joined[quad, pl.ds(pl.multiple_of(side * (alone + common), each), alone)] = merged[
        pair, pl.ds(alone_at, alone)
    ]

    def leave(g, _):
        to_partner(g).wait_send()
        return 0

    lax.fori_loop(0, pairs, leave, 0)
    series[...] = jnp.zeros(series.shape, f32)

    def finish(q):
        alone_copy(2 * q + 1 - side, q, 1 - side).wait()
        alone_copy(2 * q + side, q, side).wait()
        to_beside(q).wait_send()
        sum_copy(q, q).wait()

    in_order(finish)
    alone_copy(2 * quad + 1 - side, quad, 1 - side).wait()
    to_beside(quad).wait_send()

    local = 2 * blocks
    wide = 2 * local + REACH // LANES
    for source in range(quads):
        for b in range(0, wide, local):
            taken = min(local, wide - b)
            block = (2 * source * local + b - REACH // LANES) % outer
            here = slice(block * each, (block + taken) * each)
            series[here, :] = series[here, :] + joined[source, b * each : (b + taken) * each, :]
    stack = transform(columns(), first_ref, forward_ref, cosine, sine)
    stack_re, stack_im = stack[:, :LANES], stack[:, LANES:]
    templ_re, templ_im = templ[:, :LANES], templ[:, LANES:]
    product = jnp.concatenate(
        [stack_re * templ_re + stack_im * templ_im, stack_im * templ_re - stack_re * templ_im], axis=1
    )
    high, low = split(product)
    back = jnp.dot(jnp.concatenate([high, low, high], axis=1), back_ref[...], preferred_element_type=f32)
    turned = []
    for k in range(each):
        re = back[k * kept : (k + 1) * kept, :LANES]
        im = back[k * kept : (k + 1) * kept, LANES:]
        turned.append(jnp.concatenate([re * cosine - im * sine, re * sine + im * cosine], axis=0))
    high, low = split(jnp.concatenate(turned, axis=1))
    final = jnp.dot(last_ref[...], jnp.concatenate([high, high, low], axis=0), preferred_element_type=f32)
    for k in range(each):
        tail[pl.ds(k, count, stride=each), :] = final[:, k * LANES : (k + 1) * LANES]
    for b in range(count):
        out_ref[:, b * LANES : (b + 1) * LANES] = tail[b * each : (b + 1) * each, :] * factor


def tables(length, lags):
    outer = length // LANES
    turn = 2.0 * math.pi
    kept = (outer // 2 + 1 + 7) // 8 * 8
    weight = np.where(np.arange(kept) % (outer // 2) == 0, 1.0, 2.0) * (np.arange(kept) <= outer // 2)
    ramp = np.arange(kept)[:, None] * np.arange(outer)[None, :] % outer * (turn / outer)
    wide = np.arange(LANES)[:, None] * np.arange(LANES)[None, :] % LANES * (turn / LANES)
    twist = np.arange(kept)[:, None] * np.arange(LANES)[None, :] % length * (turn / length)
    first = split_table(np.concatenate([np.cos(ramp), -np.sin(ramp)], axis=0))
    cosine, sine = np.cos(wide), np.sin(wide)
    forward = split_table(np.block([[cosine, -sine], [sine, cosine]]))
    back = split_table(np.block([[cosine, sine], [-sine, cosine]]))
    shown = ramp[:, : lags // LANES].T
    last = split_table(np.concatenate([np.cos(shown) * weight, -np.sin(shown) * weight], axis=1))
    return (
        np.concatenate([first[0], first[1], first[0]], axis=1),
        np.concatenate([forward[0], forward[0], forward[1]], axis=0),
        np.concatenate([back[0], back[0], back[1]], axis=0),
        np.concatenate([last[0], last[1], last[0]], axis=1),
        np.stack([np.cos(twist), np.sin(twist)]).astype(np.float32),
    )


def on_device(devices, traces, templates, moveouts, masks):
    channels, width = traces.shape
    each, lags = templates.shape
    blocks = width // LANES
    outer = devices * blocks
    window = blocks + REACH // LANES
    pairs, quads = devices // 2, devices // 4
    loaded = [moveouts[None, :], masks, templates, *[jnp.asarray(table) for table in tables(outer * LANES, lags)]]
    alone, common = 2 * blocks * each, REACH // LANES * each
    return pl.pallas_call(
        functools.partial(kernel, devices, channels),
        in_specs=[pl.BlockSpec(memory_space=pl.ANY) for _ in range(len(loaded) + 1)],
        out_specs=pl.BlockSpec(memory_space=pltpu.VMEM),
        out_shape=pltpu.VMEM((each, lags), f32),
        scratch_shapes=[
            *[pltpu.VMEM(value.shape, value.dtype) for value in loaded],
            pltpu.VMEM((channels, width), f32),
            pltpu.VMEM((channels, LANES), jnp.int32),
            pltpu.VMEM((REACH // LANES // COARSE * masks.shape[0], channels), bf16),
            pltpu.VMEM((2 * channels, (blocks + COARSE) * LANES), bf16),
            pltpu.VMEM((REACH // LANES // COARSE * masks.shape[0], (blocks + COARSE) * LANES), f32),
            pltpu.VMEM((2, pairs, window * each, LANES), f32),
            pltpu.VMEM((pairs, window * each, LANES), f32),
            pltpu.VMEM((pairs, alone + common, LANES), f32),
            pltpu.VMEM((quads, common, LANES), f32),
            pltpu.VMEM((quads, 2 * alone + common, LANES), f32),
            pltpu.VMEM((outer * each, LANES), f32),
            pltpu.VMEM((lags // LANES * each, LANES), f32),
            pltpu.SemaphoreType.DMA((len(loaded),)),
            pltpu.SemaphoreType.DMA((channels // LANES,)),
            *[pltpu.SemaphoreType.DMA((count,)) for count in (pairs, pairs, quads, quads, pairs, pairs, quads, quads)],
        ],
        compiler_params=pltpu.CompilerParams(collective_id=0, has_side_effects=True),
        name="detect",
    )(*loaded[:2], traces, *loaded[2:])


def solution(mesh):
    return jax.shard_map(
        functools.partial(on_device, mesh.shape["tm"]),
        mesh=mesh,
        in_specs=(P("grp", "tm"), P("tm", None), P("grp"), P(None, "grp")),
        out_specs=P("tm", "grp"),
        check_vma=False,
    )
```
